128 devices in a mesh: eq: 8 (over x, z_hi), row: 4 (over y), col: 4 (over z_lo, core).
Axes of the slice: x: 4, y: 4, z: 4 (z_hi: 2, z_lo: 2; z = z_hi * 2 + z_lo), core: 2. Of those that a mesh axis runs over, the one named last changes fastest.
Arguments:
- transition: float32 [24576, 3072], P(('eq', 'row'), 'col'), parts along dimension 0, may hold values from -0.05 to 0.9
- covariance: float32 [24576, 3072], P(('eq', 'row'), 'col'), parts along dimension 0, may hold values from -1 to 5, as said below
Outputs:
- covariance_out: float32 [24576, 3072], P(('eq', 'row'), 'col'), parts along dimension 0
- transition_out: float32 [24576, 3072], P(('eq', 'row'), 'col'), parts along dimension 0
The draws below stay inside these ranges and needn't reach their ends.
There are 8 independent parts, one for each index of `eq`. The reference program is written for one: setup_inputs(seed, part) draws one part's arguments, and reference() takes and returns one part's arrays. A program takes and returns all parts, laid end to end along the dimension named above; each array names one. Nothing has to cross between parts.
Inputs may be any that keep to these rules, and one draw needn't show every extreme that they name: covariance is exactly symmetric.
All inputs are finite; a program needn't handle non-finite values.
Results may differ from the reference program's by a relative error of at most 0.0001.
Values sent between devices are 32-bit elements; how exact they have to be, the bound alone decides.
A program may use at most 128 MiB of HBM per device.

```python
import jax
import jax.numpy as jnp
from jax import lax

ORDER = 3072
STEPS = 1


def draw_transition(key, part):
    keys = jax.random.split(jax.random.fold_in(key, 11), 2)
    diagonal = jax.random.uniform(keys[0], (ORDER,), jnp.float32, 0.5, 0.85)
    noise = jnp.clip(jax.random.normal(keys[1], (ORDER, ORDER), jnp.float32), -6.0, 6.0) * (0.12 / ORDER ** 0.5)
    noise = jnp.clip(noise, -0.05, 0.05)
    return noise + jnp.diag(diagonal)


def draw_covariance(key, part):
    keys = jax.random.split(jax.random.fold_in(key, 23), 3)
    diagonal = jax.random.uniform(keys[0], (ORDER,), jnp.float32, 1.0, 3.0)
    normals = jnp.clip(jax.random.normal(keys[1], (ORDER, ORDER), jnp.float32), -6.0, 6.0)
    noise = jnp.clip(normals * (0.4 / (2.0 * ORDER) ** 0.5), -0.45, 0.45)
    result = noise + noise.T + jnp.diag(diagonal)
    return result


def setup_inputs(seed: int = 0, part: int = 0) -> dict:
    key_list = jax.random.split(jax.random.key(seed), 3)
    part_splits = jax.random.split(jax.random.fold_in(key_list[2], part), 3)
    transition = draw_transition(jax.random.fold_in(jax.random.fold_in(key_list[2], part), 71), part)
    covariance = draw_covariance(jax.random.fold_in(jax.random.fold_in(key_list[2], part), 71), part)
    return dict(transition=transition, covariance=covariance)


def reference(transition, covariance):
    highest = lax.Precision.HIGHEST
    matrix = transition
    current = covariance
    for repeat in range(STEPS):
        product = jnp.dot(matrix, current, precision=highest, preferred_element_type=jnp.float32)
        current = jnp.dot(product, matrix.T, precision=highest, preferred_element_type=jnp.float32) + current
        matrix = jnp.dot(matrix, matrix, precision=highest, preferred_element_type=jnp.float32)
    return current, matrix
```

```python
import jax
import jax.numpy as jnp
from jax import lax
from jax.experimental import pallas as pl
from jax.experimental.pallas import tpu as pltpu
from jax.sharding import PartitionSpec as P

N = 768
G = 256
NG = N // G
H = G // 2
BF = jnp.bfloat16
F32 = jnp.float32


def split(x):
    hi = x.astype(BF)
    lo = (x - hi.astype(F32)).astype(BF)
    return hi, lo


def dot(a, b, contract):
    return lax.dot_general(a, b, (contract, ((), ())), preferred_element_type=F32)


def dot3(ah, al, bh, bl, contract):
    return dot(ah, bh, contract) + (dot(ah, bl, contract) + dot(al, bh, contract))


NN = ((1,), (0,))
NT = ((1,), (1,))


def kernel(
    a_hbm,
    x_hbm,
    xo,
    a2,
    xcol,
    acol,
    arow,
    arh,
    arl,
    yh,
    yl,
    ch,
    cl,
    psend,
    precv,
    pkeep,
    pzrecv,
    lsem,
    rs,
    rr,
    ws,
    wr,
    ps,
    pr,
    zs,
    zr,
):
    y = lax.axis_index("row")
    c = lax.axis_index("col")
    right, left = (y + 1) % 4, (y + 3) % 4
    partner = c + 1 - 2 * (c % 2)
    other = (c + 2) % 4
    other_partner = (partner + 2) % 4

    load_a = pltpu.make_async_copy(a_hbm, acol.at[0], lsem.at[0])
    load_x = pltpu.make_async_copy(x_hbm, xcol.at[0], lsem.at[1])
    load_x.start()
    load_a.start()

    barrier = pltpu.get_barrier_semaphore()
    for where in ({"row": left}, {"row": right}, {"col": partner}, {"col": other}):
        pl.semaphore_signal(barrier, inc=1, device_id=where, device_id_type=pl.DeviceIdType.MESH)
    pl.semaphore_wait(barrier, 4)

    def remote(src, dst, send, recv, where):
        return pltpu.make_async_remote_copy(
            src_ref=src,
            dst_ref=dst,
            send_sem=send,
            recv_sem=recv,
            device_id=where,
            device_id_type=pl.DeviceIdType.MESH,
        )

    cols = (xcol, acol)

    def near(arr, d, g):
        ref = cols[arr]
        rows = pl.ds(g * G, G)
        return remote(
            ref.at[0, rows],
            ref.at[1 + d, rows],
            rs.at[arr, d, 0, g],
            rr.at[arr, d, 0, g],
            {"row": right if d == 0 else left},
        )

    def far(arr, d, g):
        ref = cols[arr]
        rows = pl.ds(g * G + d * H, H)
        return remote(
            ref.at[1 + d, rows],
            ref.at[3, rows],
            rs.at[arr, d, 1, g],
            rr.at[arr, d, 1, g],
            {"row": right if d == 0 else left},
        )

    def both(make, arr, g):
        return [make(arr, d, g) for d in range(2)]

    def start(copies):
        for copy in copies:
            copy.start()

    def arrived(copies):
        for copy in copies:
            copy.wait_recv()

    row_partner = remote(acol.at[0], arow.at[0], ws.at[0], wr.at[0], {"col": partner})

    def row_other(g):
        rows = pl.ds(g * G, G)
        return remote(acol.at[0, rows], arow.at[1, rows], ws.at[1 + g], wr.at[1 + g], {"col": other})

    def row_forward(g):
        rows = pl.ds(g * G, G)
        return remote(arow.at[1, rows], arow.at[2, rows], ws.at[4 + g], wr.at[4 + g], {"col": partner})

    load_x.wait()
    start(both(near, 0, 0))
    start(both(near, 0, 1))
    load_a.wait()
    for g in range(NG):
        row_other(g).start()
    row_partner.start()

    def convert(ref, r0, j):
        hi, lo = split(ref[pl.ds(r0, G), :])
        for k in range(NG):
            arh[j, k, pl.ds(r0, G), :] = hi[:, k * G : (k + 1) * G]
            arl[j, k, pl.ds(r0, G), :] = lo[:, k * G : (k + 1) * G]

    @pl.loop(0, NG)
    def _(g):
        convert(acol.at[0], pl.multiple_of(g * G, G), c)

    row_partner.wait_recv()

    @pl.loop(0, NG)
    def _(g):
        convert(arow.at[0], pl.multiple_of(g * G, G), partner)

    for g in range(NG):
        arrived(both(near, 0, g))
        start(both(far, 0, g))
        if g == 0:
            start(both(near, 0, 2))
        if g == 2:
            start(both(near, 1, 0))
            start(both(near, 1, 1))
        row_other(g).wait_recv()
        row_forward(g).start()
        convert(arow.at[1], g * G, other)
        row_forward(g).wait_recv()
        convert(arow.at[2], g * G, other_partner)

    def block_of(s):
        return (y + jnp.where(s == 1, 3, jnp.where(s == 2, 1, jnp.where(s == 3, 2, 0)))) % 4

    def split_group(ref, s, g):
        hi, lo = split(ref[s, pl.ds(pl.multiple_of(g * G, G), G), :])
        ch[...] = hi
        cl[...] = lo

    def add_product(out, j, g):
        @pl.loop(0, NG)
        def _(m):
            rows = pl.ds(pl.multiple_of(m * G, G), G)
            out[rows, :] += dot3(arh[j, g, rows, :], arl[j, g, rows, :], ch[...], cl[...], NN)

    def y_step(s, g):
        split_group(xcol, s, g)
        add_product(xo, block_of(s), g)

    xo[...] = jnp.zeros_like(xo)
    a2[...] = jnp.zeros_like(a2)

    @pl.loop(0, 3 * NG)
    def _(n):
        y_step(n // NG, n % NG)

    for g in range(NG):
        arrived(both(far, 0, g))

    @pl.loop(0, NG)
    def _(g):
        y_step(3, g)

    @pl.loop(0, NG)
    def _(m):
        rows = pl.ds(pl.multiple_of(m * G, G), G)
        hi, lo = split(xo[rows, :])
        yh[rows, :] = hi
        yl[rows, :] = lo

    def to_partner(q, g):
        return remote(psend.at[q, g], precv.at[q, g], ps.at[q, g], pr.at[q, g], {"col": partner})

    def to_other(g):
        return remote(pkeep.at[1, g], pzrecv.at[g], zs.at[g], zr.at[g], {"col": other})

    def step(s, g):
        j = block_of(s)
        q = (j // 2 + c // 2) % 2
        mine = (j + c) % 2 == 0
        split_group(acol, s, g)

        def p_tile(m):
            rows = pl.ds(pl.multiple_of(m * G, G), G)
            return rows, dot3(yh[rows, :], yl[rows, :], ch[...], cl[...], NT)

        @pl.when(jnp.logical_not(mine))
        def _():
            @pl.loop(0, NG)
            def _(m):
                rows, value = p_tile(m)
                psend[q, g, rows, :] = value

            to_partner(q, g).start()

        @pl.when(mine)
        def _():
            @pl.loop(0, NG)
            def _(m):
                rows, value = p_tile(m)
                pkeep[q, g, rows, :] = value

        add_product(a2, j, g)

        @pl.when(mine)
        def _():
            to_partner(q, g).wait_recv()

            @pl.loop(0, NG)
            def _(m):
                rows = pl.ds(pl.multiple_of(m * G, G), G)
                pkeep[q, g, rows, :] += precv[q, g, rows, :]

            @pl.when(q == 1)
            def _():
                to_other(g).start()

    @pl.loop(0, NG)
    def _(g):
        step(0, g)

    def near_steps(g):
        @pl.loop(1, 3)
        def _(s):
            step(s, g)

    arrived(both(near, 1, 0))
    start(both(far, 1, 0))
    start(both(near, 1, 2))
    near_steps(0)
    arrived(both(near, 1, 1))
    start(both(far, 1, 1))
    near_steps(1)
    arrived(both(far, 1, 0))
    step(3, 0)
    arrived(both(near, 1, 2))
    start(both(far, 1, 2))
    near_steps(2)
    arrived(both(far, 1, 1))
    step(3, 1)
    arrived(both(far, 1, 2))
    step(3, 2)

    for g in range(NG):
        to_other(g).wait_recv()

        @pl.loop(0, NG)
        def _(m):
            rows = pl.ds(pl.multiple_of(m * G, G), G)
            lanes = slice(g * G, (g + 1) * G)
            xo[rows, lanes] = xcol[0, rows, lanes] + (pkeep[0, g, rows, :] + pzrecv[g, rows, :])

    for arr in range(2):
        for g in range(NG):
            for copy in both(near, arr, g) + both(far, arr, g):
                copy.wait_send()
    row_partner.wait_send()
    for g in range(NG):
        row_other(g).wait_send()
        row_forward(g).wait_send()
        to_partner(0, g).wait_send()
        to_partner(1, g).wait_send()
        to_other(g).wait_send()


def solution(mesh):
    def body(a, x):
        block = jax.ShapeDtypeStruct((N, N), F32)
        vmem = pl.BlockSpec(memory_space=pltpu.VMEM)
        dma = pltpu.SemaphoreType.DMA
        xo, a2 = pl.pallas_call(
            kernel,
            out_shape=(block, block),
            in_specs=[pl.BlockSpec(memory_space=pl.ANY)] * 2,
            out_specs=(vmem, vmem),
            scratch_shapes=[
                pltpu.VMEM((4, N, N), F32),
                pltpu.VMEM((4, N, N), F32),
                pltpu.VMEM((3, N, N), F32),
                pltpu.VMEM((4, NG, N, G), BF),
                pltpu.VMEM((4, NG, N, G), BF),
                pltpu.VMEM((N, N), BF),
                pltpu.VMEM((N, N), BF),
                pltpu.VMEM((G, N), BF),
                pltpu.VMEM((G, N), BF),
                pltpu.VMEM((2, NG, N, G), F32),
                pltpu.VMEM((2, NG, N, G), F32),
                pltpu.VMEM((2, NG, N, G), F32),
                pltpu.VMEM((NG, N, G), F32),
                dma((2,)),
                dma((2, 2, 2, NG)),
                dma((2, 2, 2, NG)),
                dma((7,)),
                dma((7,)),
                dma((2, NG)),
                dma((2, NG)),
                dma((NG,)),
                dma((NG,)),
            ],
            compiler_params=pltpu.CompilerParams(
                collective_id=0, has_side_effects=True, vmem_limit_bytes=67043328
            ),
            cost_estimate=pl.CostEstimate(flops=32614907904, bytes_accessed=9437184, transcendentals=0),
        )(a, x)
        return xo, a2

    spec = P(("eq", "row"), "col")
    return jax.shard_map(
        body, mesh=mesh, in_specs=(spec, spec), out_specs=(spec, spec), check_vma=False
    )
```

```python
import jax
import jax.numpy as jnp
from jax import lax
from jax.experimental import pallas as pl
from jax.experimental.pallas import tpu as pltpu
from jax.sharding import PartitionSpec as P

N = 768
G = 256
NG = N // G
H = G // 2
BF = jnp.bfloat16
F32 = jnp.float32


def split(x):
    hi = x.astype(BF)
    lo = (x - hi.astype(F32)).astype(BF)
    return hi, lo


def dot(a, b, contract):
    return lax.dot_general(a, b, (contract, ((), ())), preferred_element_type=F32)


def dot3(ah, al, bh, bl, contract):
    return dot(ah, bh, contract) + (dot(ah, bl, contract) + dot(al, bh, contract))


NN = ((1,), (0,))
NT = ((1,), (1,))


def kernel(
    a_hbm,
    x_hbm,
    xo,
    a2,
    xcol,
    acol,
    arow,
    arh,
    arl,
    yh,
    yl,
    ch,
    cl,
    psend,
    precv,
    pkeep,
    pzrecv,
    lsem,
    rs,
    rr,
    ms,
    mr,
    ws,
    wr,
    ps,
    pr,
    zs,
    zr,
):
    y = lax.axis_index("row")
    c = lax.axis_index("col")
    partner = c + 1 - 2 * (c % 2)
    other = (c + 2) % 4
    other_partner = (partner + 2) % 4

    sign = 1 - 2 * (c % 2)
    place = ((y - c) * sign + 4) % 4
    load_a = pltpu.make_async_copy(a_hbm, acol.at[place], lsem.at[0])
    load_x = pltpu.make_async_copy(x_hbm, xcol.at[place], lsem.at[1])
    load_x.start()
    load_a.start()

    barrier = pltpu.get_barrier_semaphore()
    for where in ({"row": (y + 1) % 4}, {"row": (y + 3) % 4}, {"col": partner}, {"col": other}):
        pl.semaphore_signal(barrier, inc=1, device_id=where, device_id_type=pl.DeviceIdType.MESH)
    pl.semaphore_wait(barrier, 4)

    def remote(src, dst, send, recv, where):
        return pltpu.make_async_remote_copy(
            src_ref=src,
            dst_ref=dst,
            send_sem=send,
            recv_sem=recv,
            device_id=where,
            device_id_type=pl.DeviceIdType.MESH,
        )

    cols = (xcol, acol)

    fwd, bwd = (y + sign + 4) % 4, (y - sign + 4) % 4
    before, after, across = (place + 3) % 4, (place + 1) % 4, (place + 2) % 4
    ends = place % 2 == 1

    def ring(arr, d, kind, g, slot, r0, size):
        rows = pl.ds(r0, size)
        return remote(
            cols[arr].at[slot, rows],
            cols[arr].at[slot, rows],
            rs.at[arr, d, kind, g],
            rr.at[arr, d, kind, g],
            {"row": fwd if d == 0 else bwd},
        )

    def near(arr, d, g):
        return ring(arr, d, 0, g, place, g * G, G)

    def far(arr, d, g):
        return ring(arr, d, 1, g, before if d == 0 else after, g * G + d * H, H)

    def near_in(arr, d, g):
        return ring(arr, d, 0, g, before if d == 0 else after, g * G, G)

    def far_in(arr, d, g):
        return ring(arr, d, 1, g, across, g * G + d * H, H)

    def whole(g, inward):
        return ring(0, 0, 1, g, across if inward else before, g * G, G)

    def both(make, arr, g):
        return [make(arr, d, g) for d in range(2)]

    def start(copies):
        for copy in copies:
            copy.start()

    def arrived(copies):
        for copy in copies:
            copy.wait_recv()

    def mate(g):
        rows = pl.ds(g * G, G)
        return remote(xcol.at[1, rows], xcol.at[1, rows], ms.at[g], mr.at[g], {"col": partner})

    def x_near(act, g):
        act(near(0, 0, g))

        @pl.when(place != 1)
        def _():
            act(near(0, 1, g))

    def x_far(act, g):
        @pl.when(ends)
        def _():
            for copy in both(far, 0, g):
                act(copy)

        @pl.when(place == 0)
        def _():
            act(whole(g, False))

    def x_near_in(g):
        near_in(0, 0, g).wait_recv()

        @pl.when(place != 0)
        def _():
            near_in(0, 1, g).wait_recv()

        @pl.when(place == 0)
        def _():
            mate(g).wait_recv()

        @pl.when(place == 2)
        def _():
            mate(g).start()

    def x_far_in(g):
        @pl.when(place % 2 == 0)
        def _():
            for copy in both(far_in, 0, g):
                copy.wait_recv()

        @pl.when(place == 1)
        def _():
            whole(g, True).wait_recv()

        @pl.when(place == 3)
        def _():
            mate(g).wait_recv()

    def begin(copy):
        copy.start()

    row_partner = remote(acol.at[place], arow.at[0], ws.at[0], wr.at[0], {"col": partner})

    def row_other(g):
        rows = pl.ds(g * G, G)
        return remote(acol.at[place, rows], arow.at[1, rows], ws.at[1 + g], wr.at[1 + g], {"col": other})

    def row_forward(g):
        rows = pl.ds(g * G, G)
        return remote(arow.at[1, rows], arow.at[2, rows], ws.at[4 + g], wr.at[4 + g], {"col": partner})

    load_x.wait()
    x_near(begin, 0)
    x_near(begin, 1)

    @pl.when(place == 1)
    def _():
        for g in range(NG):
            mate(g).start()

    load_a.wait()
    for g in range(NG):
        row_other(g).start()
    row_partner.start()

    def convert(ref, r0, j):
        hi, lo = split(ref[pl.ds(r0, G), :])
        for k in range(NG):
            arh[j, k, pl.ds(r0, G), :] = hi[:, k * G : (k + 1) * G]
            arl[j, k, pl.ds(r0, G), :] = lo[:, k * G : (k + 1) * G]

    @pl.loop(0, NG)
    def _(g):
        convert(acol.at[place], pl.multiple_of(g * G, G), c)

    row_partner.wait_recv()

    @pl.loop(0, NG)
    def _(g):
        convert(arow.at[0], pl.multiple_of(g * G, G), partner)

    for g in range(NG):
        x_near_in(g)
        x_far(begin, g)
        if g == 0:
            x_near(begin, 2)
        if g == 2:
            start(both(near, 1, 0))
            start(both(near, 1, 1))
        row_other(g).wait_recv()
        row_forward(g).start()
        convert(arow.at[1], g * G, other)
        row_forward(g).wait_recv()
        convert(arow.at[2], g * G, other_partner)

    def block_of(s):
        return (c + sign * s + 4) % 4

    def split_group(ref, s, g):
        hi, lo = split(ref[s, pl.ds(pl.multiple_of(g * G, G), G), :])
        ch[...] = hi
        cl[...] = lo

    def add_product(out, j, g):
        @pl.loop(0, NG)
        def _(m):
            rows = pl.ds(pl.multiple_of(m * G, G), G)
            out[rows, :] += dot3(arh[j, g, rows, :], arl[j, g, rows, :], ch[...], cl[...], NN)

    def y_step(s, g):
        split_group(xcol, s, g)
        flipped = jnp.logical_and(s == 1, place % 3 == 0)

        @pl.when(jnp.logical_not(flipped))
        def _():
            add_product(xo, block_of(s), g)

        @pl.when(flipped)
        def _():
            j = block_of(s)
            lanes = pl.ds(pl.multiple_of(g * G, G), G)

            @pl.loop(0, NG)
            def _(m):
                rows = pl.ds(pl.multiple_of(m * G, G), G)
                total = xo[rows, lanes]
                for k in range(NG):
                    part = slice(k * G, (k + 1) * G)
                    total += dot3(arh[j, k, rows, :], arl[j, k, rows, :], ch[:, part], cl[:, part], NT)
                xo[rows, lanes] = total

    xo[...] = jnp.zeros_like(xo)
    a2[...] = jnp.zeros_like(a2)

    @pl.loop(0, 3 * NG)
    def _(n):
        y_step((place + 3 + n // NG) % 4, n % NG)

    for g in range(NG):
        x_far_in(g)

    @pl.loop(0, NG)
    def _(g):
        y_step(across, g)

    @pl.loop(0, NG)
    def _(m):
        rows = pl.ds(pl.multiple_of(m * G, G), G)
        hi, lo = split(xo[rows, :])
        yh[rows, :] = hi
        yl[rows, :] = lo

    def to_partner(q, g):
        return remote(psend.at[q, g], precv.at[q, g], ps.at[q, g], pr.at[q, g], {"col": partner})

    def to_other(g):
        return remote(pkeep.at[1, g], pzrecv.at[g], zs.at[g], zr.at[g], {"col": other})

    def step(s, g):
        j = block_of(s)
        q = (j // 2 + c // 2) % 2
        mine = (j + c) % 2 == 0
        split_group(acol, s, g)

        def p_tile(m):
            rows = pl.ds(pl.multiple_of(m * G, G), G)
            return rows, dot3(yh[rows, :], yl[rows, :], ch[...], cl[...], NT)

        @pl.when(jnp.logical_not(mine))
        def _():
            @pl.loop(0, NG)
            def _(m):
                rows, value = p_tile(m)
                psend[q, g, rows, :] = value

            to_partner(q, g).start()

        @pl.when(mine)
        def _():
            @pl.loop(0, NG)
            def _(m):
                rows, value = p_tile(m)
                pkeep[q, g, rows, :] = value

        add_product(a2, j, g)

        @pl.when(mine)
        def _():
            to_partner(q, g).wait_recv()

            @pl.loop(0, NG)
            def _(m):
                rows = pl.ds(pl.multiple_of(m * G, G), G)
                pkeep[q, g, rows, :] += precv[q, g, rows, :]

            @pl.when(q == 1)
            def _():
                to_other(g).start()

    @pl.loop(0, NG)
    def _(g):
        step(place, g)

    def near_steps(g):
        @pl.loop(0, 2)
        def _(n):
            step((place + 3 + 2 * n) % 4, g)

    arrived(both(near_in, 1, 0))
    start(both(far, 1, 0))
    start(both(near, 1, 2))
    near_steps(0)
    arrived(both(near_in, 1, 1))
    start(both(far, 1, 1))
    near_steps(1)
    arrived(both(far_in, 1, 0))
    step(across, 0)
    arrived(both(near_in, 1, 2))
    start(both(far, 1, 2))
    near_steps(2)
    arrived(both(far_in, 1, 1))
    step(across, 1)
    arrived(both(far_in, 1, 2))
    step(across, 2)

    for g in range(NG):
        to_other(g).wait_recv()

        @pl.loop(0, NG)
        def _(m):
            rows = pl.ds(pl.multiple_of(m * G, G), G)
            lanes = slice(g * G, (g + 1) * G)
            xo[rows, lanes] = xcol[place, rows, lanes] + (pkeep[0, g, rows, :] + pzrecv[g, rows, :])

    def sent(copy):
        copy.wait_send()

    for g in range(NG):
        x_near(sent, g)
        x_far(sent, g)
        for copy in both(near, 1, g) + both(far, 1, g):
            copy.wait_send()

    @pl.when(jnp.logical_or(place == 1, place == 2))
    def _():
        for g in range(NG):
            mate(g).wait_send()

    row_partner.wait_send()
    for g in range(NG):
        row_other(g).wait_send()
        row_forward(g).wait_send()
        to_partner(0, g).wait_send()
        to_partner(1, g).wait_send()
        to_other(g).wait_send()


def solution(mesh):
    def body(a, x):
        block = jax.ShapeDtypeStruct((N, N), F32)
        vmem = pl.BlockSpec(memory_space=pltpu.VMEM)
        dma = pltpu.SemaphoreType.DMA
        xo, a2 = pl.pallas_call(
            kernel,
            out_shape=(block, block),
            in_specs=[pl.BlockSpec(memory_space=pl.ANY)] * 2,
            out_specs=(vmem, vmem),
            scratch_shapes=[
                pltpu.VMEM((4, N, N), F32),
                pltpu.VMEM((4, N, N), F32),
                pltpu.VMEM((3, N, N), F32),
                pltpu.VMEM((4, NG, N, G), BF),
                pltpu.VMEM((4, NG, N, G), BF),
                pltpu.VMEM((N, N), BF),
                pltpu.VMEM((N, N), BF),
                pltpu.VMEM((G, N), BF),
                pltpu.VMEM((G, N), BF),
                pltpu.VMEM((2, NG, N, G), F32),
                pltpu.VMEM((2, NG, N, G), F32),
                pltpu.VMEM((2, NG, N, G), F32),
                pltpu.VMEM((NG, N, G), F32),
                dma((2,)),
                dma((2, 2, 2, NG)),
                dma((2, 2, 2, NG)),
                dma((NG,)),
                dma((NG,)),
                dma((7,)),
                dma((7,)),
                dma((2, NG)),
                dma((2, NG)),
                dma((NG,)),
                dma((NG,)),
            ],
            compiler_params=pltpu.CompilerParams(
                collective_id=0, has_side_effects=True, vmem_limit_bytes=67043328
            ),
            cost_estimate=pl.CostEstimate(flops=32614907904, bytes_accessed=9437184, transcendentals=0),
        )(a, x)
        return xo, a2

    spec = P(("eq", "row"), "col")
    return jax.shard_map(
        body, mesh=mesh, in_specs=(spec, spec), out_specs=(spec, spec), check_vma=False
    )
```

```python
import jax
import jax.numpy as jnp
from jax import lax
from jax.experimental import pallas as pl
from jax.experimental.pallas import tpu as pltpu
from jax.sharding import PartitionSpec as P

N = 768
G = 256
NG = N // G
H = G // 2
NU = 2 * NG
BF = jnp.bfloat16
F32 = jnp.float32


def split(x):
    hi = x.astype(BF)
    lo = (x - hi.astype(F32)).astype(BF)
    return hi, lo


def dot(a, b, contract):
    return lax.dot_general(a, b, (contract, ((), ())), preferred_element_type=F32)


def dot3(ah, al, bh, bl, contract):
    return dot(ah, bh, contract) + (dot(ah, bl, contract) + dot(al, bh, contract))


NN = ((1,), (0,))
NT = ((1,), (1,))


def kernel(
    a_hbm,
    x_hbm,
    xo_hbm,
    a2_hbm,
    xo,
    a2,
    xcol,
    acol,
    arow,
    arh,
    arl,
    yh,
    yl,
    ch,
    cl,
    part,
    precv,
    pzrecv,
    lsem,
    osem,
    rs,
    rr,
    ns,
    nr,
    ms,
    mr,
    ws,
    wr,
    ps,
    pr,
    zs,
    zr,
):
    y = lax.axis_index("row")
    c = lax.axis_index("col")
    partner = c + 1 - 2 * (c % 2)
    other = (c + 2) % 4
    other_partner = (partner + 2) % 4

    sign = 1 - 2 * (c % 2)
    place = ((y - c) * sign + 4) % 4
    load_a = pltpu.make_async_copy(a_hbm, acol.at[place], lsem.at[0])
    load_x = pltpu.make_async_copy(x_hbm, xcol.at[place], lsem.at[1])
    load_x.start()
    load_a.start()

    barrier = pltpu.get_barrier_semaphore()
    for where in ({"row": (y + 1) % 4}, {"row": (y + 3) % 4}, {"col": partner}, {"col": other}):
        pl.semaphore_signal(barrier, inc=1, device_id=where, device_id_type=pl.DeviceIdType.MESH)
    pl.semaphore_wait(barrier, 4)

    def remote(src, dst, send, recv, where):
        return pltpu.make_async_remote_copy(
            src_ref=src,
            dst_ref=dst,
            send_sem=send,
            recv_sem=recv,
            device_id=where,
            device_id_type=pl.DeviceIdType.MESH,
        )

    fwd, bwd = (y + sign + 4) % 4, (y - sign + 4) % 4
    before, after, across = (place + 3) % 4, (place + 1) % 4, (place + 2) % 4

    def ring(d, kind, g, slot, r0, size):
        rows = xcol.at[slot, pl.ds(r0, size)]
        return remote(rows, rows, rs.at[d, kind, g], rr.at[d, kind, g], {"row": fwd if d == 0 else bwd})

    def near(d, g):
        return ring(d, 0, g, place, g * G, G)

    def far(d, g):
        return ring(d, 1, g, before if d == 0 else after, g * G + d * H, H)

    def near_in(d, g):
        return ring(d, 0, g, before if d == 0 else after, g * G, G)

    def far_in(d, g):
        return ring(d, 1, g, across, g * G + d * H, H)

    def whole(g, inward):
        return ring(1, 1, g, across if inward else after, g * G, G)

    def a_ring(d, i, slot):
        half = (d + c + (i % 4) // 2) % 2
        r0 = pl.multiple_of(half * (NG * H), H) + (i % 2) * G
        rows = acol.at[slot, pl.ds(r0, G - (i % 2) * H)]
        return remote(rows, rows, ns.at[d, i], nr.at[d, i], {"row": fwd if d == 0 else bwd})

    def a_out(i):
        slots = (before, after) if i >= 4 else (place, place)
        return [a_ring(d, i, slots[d]) for d in range(2)]

    def a_in(i):
        slots = (across, across) if i >= 4 else (before, after)
        return [a_ring(d, i, slots[d]) for d in range(2)]

    def both(make, g):
        return [make(d, g) for d in range(2)]

    def start(copies):
        for copy in copies:
            copy.start()

    def arrived(copies):
        for copy in copies:
            copy.wait_recv()

    def mate(g):
        rows = pl.ds(g * G, G)
        return remote(xcol.at[1, rows], xcol.at[1, rows], ms.at[g], mr.at[g], {"col": partner})

    def x_near(act, g):
        act(near(0, g))

        @pl.when(place != 1)
        def _():
            act(near(1, g))

    def x_far(act, g):
        @pl.when(place < 2)
        def _():
            act(far(0, g))

        @pl.when(place >= 2)
        def _():
            act(far(1, g))

        @pl.when(place == 1)
        def _():
            act(whole(g, False))

    def x_near_in(g):
        near_in(0, g).wait_recv()

        @pl.when(place != 0)
        def _():
            near_in(1, g).wait_recv()

        @pl.when(place == 0)
        def _():
            mate(g).wait_recv()

        @pl.when(place == 2)
        def _():
            mate(g).start()

    def x_far_in(g):
        @pl.when(jnp.logical_or(place == 1, place == 2))
        def _():
            for copy in both(far_in, g):
                copy.wait_recv()

        @pl.when(place == 0)
        def _():
            whole(g, True).wait_recv()

        @pl.when(place == 3)
        def _():
            mate(g).wait_recv()

    def begin(copy):
        copy.start()

    row_partner = remote(acol.at[place], arow.at[0], ws.at[0], wr.at[0], {"col": partner})

    def row_other(g):
        rows = pl.ds(g * G, G)
        return remote(acol.at[place, rows], arow.at[1, rows], ws.at[1 + g], wr.at[1 + g], {"col": other})

    def row_forward(g):
        rows = pl.ds(g * G, G)
        return remote(arow.at[1, rows], arow.at[2, rows], ws.at[4 + g], wr.at[4 + g], {"col": partner})

    load_x.wait()
    for g in range(NG):
        x_near(begin, g)

    @pl.when(place == 1)
    def _():
        for g in range(NG):
            mate(g).start()

    load_a.wait()
    for g in range(NG):
        row_other(g).start()
    row_partner.start()

    def convert(ref, r0, j):
        hi, lo = split(ref[pl.ds(r0, G), :])
        for k in range(NU):
            arh[j, k, pl.ds(r0, G), :] = hi[:, k * H : (k + 1) * H]
            arl[j, k, pl.ds(r0, G), :] = lo[:, k * H : (k + 1) * H]

    @pl.loop(0, NG)
    def _(g):
        convert(acol.at[place], pl.multiple_of(g * G, G), c)

    row_partner.wait_recv()

    @pl.loop(0, NG)
    def _(g):
        convert(arow.at[0], pl.multiple_of(g * G, G), partner)

    def block_of(s):
        return (c + sign * s + 4) % 4

    def pair(ref, j, u):
        return jnp.concatenate([ref[j, u[0]], ref[j, u[1]]], axis=1)

    def split_unit(ref, s, u, at):
        hi, lo = split(ref[s, pl.ds(pl.multiple_of(u * H, H), H), :])
        ch[at * H : (at + 1) * H, :] = hi
        cl[at * H : (at + 1) * H, :] = lo

    def split_units(ref, s, u):
        split_unit(ref, s, u[0], 0)
        split_unit(ref, s, u[1], 1)

    def lanes_of(n):
        return pl.ds(pl.multiple_of(n * G, G), G)

    def add_product(out, j, u):
        @pl.loop(0, NG)
        def _(n):
            lanes = lanes_of(n)
            out[:, lanes] += dot3(pair(arh, j, u), pair(arl, j, u), ch[:, lanes], cl[:, lanes], NN)

    def y_step(s, g):
        with jax.named_scope("y"):
            u = (2 * g, 2 * g + 1)
            split_units(xcol, s, u)
            flipped = jnp.logical_and(s == 1, place % 3 == 0)
            j = block_of(s)

            @pl.when(jnp.logical_not(flipped))
            def _():
                add_product(xo, j, u)

            @pl.when(flipped)
            def _():
                @pl.loop(0, NG)
                def _(k):
                    v = (2 * k, 2 * k + 1)
                    lanes = lanes_of(k)
                    xo[:, lanes_of(g)] += dot3(pair(arh, j, v), pair(arl, j, v), ch[:, lanes], cl[:, lanes], NT)

    def y_near(g):
        @pl.loop(0, 2)
        def _(n):
            y_step((place + 3 + 2 * n) % 4, g)

    def row_in(g):
        with jax.named_scope("row"):
            row_other(g).wait_recv()
            row_forward(g).start()
            convert(arow.at[1], g * G, other)
            row_forward(g).wait_recv()
            convert(arow.at[2], g * G, other_partner)

    xo[...] = jnp.zeros_like(xo)
    a2[...] = jnp.zeros_like(a2)

    with jax.named_scope("x0"):
        x_near_in(0)
    x_far(begin, 0)
    row_in(0)
    with jax.named_scope("x1"):
        x_near_in(1)
    x_far(begin, 1)
    row_in(1)
    row_in(2)

    with jax.named_scope("x2"):
        x_near_in(2)
    x_far(begin, 2)

    heavy = place // 2

    def a_begin(which):
        for d in range(2):

            @pl.when(which == d)
            def _():
                a_ring(d, 0, place).start()
                a_ring(d, 1, place).start()

    a_begin(heavy)

    @pl.loop(0, NG)
    def _(g):
        y_step(place, g)

    y_near(0)
    a_begin(1 - heavy)

    @pl.loop(1, NG)
    def _(g):
        y_near(g)

    with jax.named_scope("xfar"):
        for g in range(NG):
            x_far_in(g)

    @pl.loop(0, NG)
    def _(g):
        y_step(across, g)

    @pl.loop(0, NG)
    def _(m):
        rows = pl.ds(pl.multiple_of(m * G, G), G)
        hi, lo = split(xo[rows, :])
        yh[rows, :] = hi
        yl[rows, :] = lo

    pieces = ((0, 2), (2, 1), (3, 2), (5, 1))
    low, high, rest = (0, 1), (3, 4), (2, 5)
    left, right = (place + 4 - sign) % 4, (place + 4 + sign) % 4

    def to_partner(q, i):
        u = pl.ds(*pieces[i])
        return remote(part.at[q, u], precv.at[q, u], ps.at[q, i], pr.at[q, i], {"col": partner})

    def to_other(i):
        u = pl.ds(*pieces[i])
        return remote(part.at[3, u], pzrecv.at[u], zs.at[i], zr.at[i], {"col": other})

    def role(s):
        j = block_of(s)
        q = (j // 2 + c // 2) % 2
        return q, (j + c) % 2 == 0

    def partial(s, u):
        with jax.named_scope("p"):
            for k in range(2):
                split_unit(acol, s[k], u[k], k)
            value = dot3(yh[...], yl[...], ch[...], cl[...], NT)
            for k in range(2):
                q, mine = role(s[k])
                part[q + 2 * mine.astype(jnp.int32), u[k]] = value[:, k * H : (k + 1) * H]

    def hand_over(s, i):
        q, mine = role(s)

        @pl.when(jnp.logical_not(mine))
        def _():
            to_partner(q, i).start()

    def collect(s, i):
        q, mine = role(s)
        u0, n = pieces[i]

        @pl.when(mine)
        def _():
            with jax.named_scope("pwait"):
                to_partner(q, i).wait_recv()
            part[2 + q, u0 : u0 + n] += precv[q, u0 : u0 + n]

            @pl.when(q == 1)
            def _():
                to_other(i).start()

    def square(s, u):
        with jax.named_scope("a2"):
            split_units(acol, s, u)
            add_product(a2, block_of(s), u)

    def side(n):
        return (place + 4 + (2 * n - 1) * sign) % 4

    def twice(f):
        @pl.loop(0, 2)
        def _(n):
            f(n)

    def ends(u0):
        return (u0, u0 + 1)

    def over(*items):
        for item in items:
            hand_over(*item)

    def gather(*items):
        for item in items:
            collect(*item)

    def arrive(i):
        with jax.named_scope("ring"):
            arrived(a_in(i))

    twice(lambda n: partial((place, place), ends(3 * n)))
    over((place, 0), (place, 2))
    partial((place, place), rest)
    over((place, 1), (place, 3))
    square(place, low)
    gather((place, 0), (place, 2), (place, 1), (place, 3))
    square(place, high)

    arrive(0)
    start(a_out(4))
    start(a_out(2))
    twice(lambda n: partial((side(n), side(n)), ends(3 * n)))
    over((left, 0), (right, 2))
    square(place, rest)
    gather((left, 0), (right, 2))

    arrive(1)
    start(a_out(5))
    start(a_out(3))
    partial((left, right), rest)
    over((left, 1), (right, 3))
    twice(lambda n: square(side(n), ends(3 * n)))
    gather((left, 1), (right, 3))

    arrive(4)
    twice(lambda n: partial((across, across), ends(3 * n)))
    over((across, 0), (across, 2))
    square(across, low)
    gather((across, 0), (across, 2))
    square(across, high)

    arrive(2)
    twice(lambda n: partial((side(n), side(n)), ends(3 - 3 * n)))
    over((left, 2), (right, 0))
    square(left, high)
    gather((left, 2), (right, 0))

    arrive(5)
    partial((across, across), rest)
    over((across, 1), (across, 3))
    square(right, low)
    gather((across, 1), (across, 3))

    arrive(3)
    partial((left, right), (5, 2))
    over((left, 3), (right, 1))
    square(across, rest)
    gather((left, 3), (right, 1))
    twice(lambda n: square(side(n), rest))

    a2_out = pltpu.make_async_copy(a2, a2_hbm, lsem.at[0])
    a2_out.start()

    def xo_out(i):
        lanes = pl.ds(pieces[i][0] * H, pieces[i][1] * H)
        return pltpu.make_async_copy(xo.at[:, lanes], xo_hbm.at[:, lanes], osem.at[i])

    for i in (0, 2, 1, 3):
        u0, n = pieces[i]
        with jax.named_scope("z"):
            to_other(i).wait_recv()

        for u in range(u0, u0 + n):
            lanes = slice(u * H, (u + 1) * H)
            xo[:, lanes] = xcol[place, :, lanes] + (part[2, u] + pzrecv[u])

        xo_out(i).start()

    def sent(copy):
        copy.wait_send()

    for g in range(NG):
        x_near(sent, g)
        x_far(sent, g)
        row_other(g).wait_send()
        row_forward(g).wait_send()

    for i in range(6):
        for copy in a_out(i):
            copy.wait_send()

    for i in range(4):
        to_partner(0, i).wait_send()
        to_partner(1, i).wait_send()
        to_other(i).wait_send()

    @pl.when(jnp.logical_or(place == 1, place == 2))
    def _():
        for g in range(NG):
            mate(g).wait_send()

    row_partner.wait_send()
    a2_out.wait()
    for i in range(4):
        xo_out(i).wait()


def solution(mesh):
    def body(a, x):
        block = jax.ShapeDtypeStruct((N, N), F32)
        dma = pltpu.SemaphoreType.DMA
        xo, a2 = pl.pallas_call(
            kernel,
            out_shape=(block, block),
            in_specs=[pl.BlockSpec(memory_space=pl.ANY)] * 2,
            out_specs=[pl.BlockSpec(memory_space=pl.ANY)] * 2,
            scratch_shapes=[
                pltpu.VMEM((N, N), F32),
                pltpu.VMEM((N, N), F32),
                pltpu.VMEM((4, N, N), F32),
                pltpu.VMEM((4, N, N), F32),
                pltpu.VMEM((3, N, N), F32),
                pltpu.VMEM((4, NU, N, H), BF),
                pltpu.VMEM((4, NU, N, H), BF),
                pltpu.VMEM((N, N), BF),
                pltpu.VMEM((N, N), BF),
                pltpu.VMEM((G, N), BF),
                pltpu.VMEM((G, N), BF),
                pltpu.VMEM((4, NU, N, H), F32),
                pltpu.VMEM((2, NU, N, H), F32),
                pltpu.VMEM((NU, N, H), F32),
                dma((2,)),
                dma((4,)),
                dma((2, 2, NG)),
                dma((2, 2, NG)),
                dma((2, 6)),
                dma((2, 6)),
                dma((NG,)),
                dma((NG,)),
                dma((7,)),
                dma((7,)),
                dma((2, 4)),
                dma((2, 4)),
                dma((4,)),
                dma((4,)),
            ],
            compiler_params=pltpu.CompilerParams(
                collective_id=0, has_side_effects=True, vmem_limit_bytes=67043328
            ),
            cost_estimate=pl.CostEstimate(flops=32614907904, bytes_accessed=9437184, transcendentals=0),
        )(a, x)
        return xo, a2

    spec = P(("eq", "row"), "col")
    return jax.shard_map(
        body, mesh=mesh, in_specs=(spec, spec), out_specs=(spec, spec), check_vma=False
    )
```

```python
import jax
import jax.numpy as jnp
from jax import lax
from jax.experimental import pallas as pl
from jax.experimental.pallas import tpu as pltpu
from jax.sharding import PartitionSpec as P

N = 768
G = 256
NG = N // G
H = G // 2
NU = 2 * NG
BF = jnp.bfloat16
F32 = jnp.float32


def split(x):
    hi = x.astype(BF)
    lo = (x - hi.astype(F32)).astype(BF)
    return hi, lo


def dot(a, b, contract):
    return lax.dot_general(a, b, (contract, ((), ())), preferred_element_type=F32)


def dot3(ah, al, bh, bl, contract):
    return dot(ah, bh, contract) + (dot(ah, bl, contract) + dot(al, bh, contract))


NN = ((1,), (0,))
NT = ((1,), (1,))


def kernel(
    a_hbm,
    x_hbm,
    xo,
    a2,
    xcol,
    acol,
    arow,
    arh,
    arl,
    yh,
    yl,
    ch,
    cl,
    part,
    precv,
    pzrecv,
    lsem,
    rs,
    rr,
    ns,
    nr,
    ms,
    mr,
    ws,
    wr,
    ps,
    pr,
    zs,
    zr,
):
    y = lax.axis_index("row")
    c = lax.axis_index("col")
    partner = c + 1 - 2 * (c % 2)
    other = (c + 2) % 4
    other_partner = (partner + 2) % 4

    sign = 1 - 2 * (c % 2)
    place = ((y - c) * sign + 4) % 4
    load_a = pltpu.make_async_copy(a_hbm, acol.at[place], lsem.at[0])
    load_x = pltpu.make_async_copy(x_hbm, xcol.at[place], lsem.at[1])
    load_x.start()
    load_a.start()

    barrier = pltpu.get_barrier_semaphore()
    for where in ({"row": (y + 1) % 4}, {"row": (y + 3) % 4}, {"col": partner}, {"col": other}):
        pl.semaphore_signal(barrier, inc=1, device_id=where, device_id_type=pl.DeviceIdType.MESH)
    pl.semaphore_wait(barrier, 4)

    def remote(src, dst, send, recv, where):
        return pltpu.make_async_remote_copy(
            src_ref=src,
            dst_ref=dst,
            send_sem=send,
            recv_sem=recv,
            device_id=where,
            device_id_type=pl.DeviceIdType.MESH,
        )

    fwd, bwd = (y + sign + 4) % 4, (y - sign + 4) % 4
    before, after, across = (place + 3) % 4, (place + 1) % 4, (place + 2) % 4

    def ring(d, kind, g, slot, r0, size):
        rows = xcol.at[slot, pl.ds(r0, size)]
        return remote(rows, rows, rs.at[d, kind, g], rr.at[d, kind, g], {"row": fwd if d == 0 else bwd})

    def near(d, g):
        return ring(d, 0, g, place, g * G, G)

    def far(d, g):
        return ring(d, 1, g, before if d == 0 else after, g * G + d * H, H)

    def near_in(d, g):
        return ring(d, 0, g, before if d == 0 else after, g * G, G)

    def far_in(d, g):
        return ring(d, 1, g, across, g * G + d * H, H)

    def whole(g, inward):
        return ring(1, 1, g, across if inward else after, g * G, G)

    def a_ring(d, i, slot):
        half = (d + c + (1 if 3 <= i < 6 else 0)) % 2
        rows = acol.at[slot, pl.ds(pl.multiple_of(half * (NG * H), H) + (i % 3) * H, H)]
        return remote(rows, rows, ns.at[d, i], nr.at[d, i], {"row": fwd if d == 0 else bwd})

    def a_out(i):
        slots = (before, after) if i >= 6 else (place, place)
        return [a_ring(d, i, slots[d]) for d in range(2)]

    def a_in(i):
        slots = (across, across) if i >= 6 else (before, after)
        return [a_ring(d, i, slots[d]) for d in range(2)]

    def both(make, g):
        return [make(d, g) for d in range(2)]

    def start(copies):
        for copy in copies:
            copy.start()

    def arrived(copies):
        for copy in copies:
            copy.wait_recv()

    def mate(g):
        rows = pl.ds(g * G, G)
        return remote(xcol.at[1, rows], xcol.at[1, rows], ms.at[g], mr.at[g], {"col": partner})

    def x_near(act, g):
        act(near(0, g))

        @pl.when(place != 1)
        def _():
            act(near(1, g))

    def x_far(act, g):
        @pl.when(place < 2)
        def _():
            act(far(0, g))

        @pl.when(place >= 2)
        def _():
            act(far(1, g))

        @pl.when(place == 1)
        def _():
            act(whole(g, False))

    def x_near_in(g):
        near_in(0, g).wait_recv()

        @pl.when(place != 0)
        def _():
            near_in(1, g).wait_recv()

        @pl.when(place == 0)
        def _():
            mate(g).wait_recv()

        @pl.when(place == 2)
        def _():
            mate(g).start()

    def x_far_in(g):
        @pl.when(jnp.logical_or(place == 1, place == 2))
        def _():
            for copy in both(far_in, g):
                copy.wait_recv()

        @pl.when(place == 0)
        def _():
            whole(g, True).wait_recv()

        @pl.when(place == 3)
        def _():
            mate(g).wait_recv()

    def begin(copy):
        copy.start()

    row_partner = remote(acol.at[place], arow.at[0], ws.at[0], wr.at[0], {"col": partner})

    def row_other(g):
        rows = pl.ds(g * G, G)
        return remote(acol.at[place, rows], arow.at[1, rows], ws.at[1 + g], wr.at[1 + g], {"col": other})

    def row_forward(g):
        rows = pl.ds(g * G, G)
        return remote(arow.at[1, rows], arow.at[2, rows], ws.at[4 + g], wr.at[4 + g], {"col": partner})

    load_x.wait()
    for g in range(NG):
        x_near(begin, g)

    @pl.when(place == 1)
    def _():
        for g in range(NG):
            mate(g).start()

    load_a.wait()
    for g in range(NG):
        row_other(g).start()
    row_partner.start()

    def convert(ref, r0, j):
        hi, lo = split(ref[pl.ds(r0, G), :])
        for k in range(NU):
            arh[j, k, pl.ds(r0, G), :] = hi[:, k * H : (k + 1) * H]
            arl[j, k, pl.ds(r0, G), :] = lo[:, k * H : (k + 1) * H]

    @pl.loop(0, NG)
    def _(g):
        convert(acol.at[place], pl.multiple_of(g * G, G), c)

    row_partner.wait_recv()

    @pl.loop(0, NG)
    def _(g):
        convert(arow.at[0], pl.multiple_of(g * G, G), partner)

    def block_of(s):
        return (c + sign * s + 4) % 4

    def pair(ref, j, u):
        return jnp.concatenate([ref[j, u[0]], ref[j, u[1]]], axis=1)

    def split_unit(ref, s, u, at):
        hi, lo = split(ref[s, pl.ds(pl.multiple_of(u * H, H), H), :])
        ch[at * H : (at + 1) * H, :] = hi
        cl[at * H : (at + 1) * H, :] = lo

    def split_units(ref, s, u):
        split_unit(ref, s, u[0], 0)
        split_unit(ref, s, u[1], 1)

    def lanes_of(n):
        return pl.ds(pl.multiple_of(n * G, G), G)

    def add_product(out, j, u):
        @pl.loop(0, NG)
        def _(n):
            lanes = lanes_of(n)
            out[:, lanes] += dot3(pair(arh, j, u), pair(arl, j, u), ch[:, lanes], cl[:, lanes], NN)

    def y_step(s, g):
        with jax.named_scope("y"):
            u = (2 * g, 2 * g + 1)
            split_units(xcol, s, u)
            flipped = jnp.logical_and(s == 1, place % 3 == 0)
            j = block_of(s)

            @pl.when(jnp.logical_not(flipped))
            def _():
                add_product(xo, j, u)

            @pl.when(flipped)
            def _():
                @pl.loop(0, NG)
                def _(k):
                    v = (2 * k, 2 * k + 1)
                    lanes = lanes_of(k)
                    xo[:, lanes_of(g)] += dot3(pair(arh, j, v), pair(arl, j, v), ch[:, lanes], cl[:, lanes], NT)

    def y_near(g):
        @pl.loop(0, 2)
        def _(n):
            y_step((place + 3 + 2 * n) % 4, g)

    def row_in(g):
        with jax.named_scope("row"):
            row_other(g).wait_recv()
            row_forward(g).start()
            convert(arow.at[1], g * G, other)
            row_forward(g).wait_recv()
            convert(arow.at[2], g * G, other_partner)

    xo[...] = jnp.zeros_like(xo)
    a2[...] = jnp.zeros_like(a2)

    with jax.named_scope("x0"):
        x_near_in(0)
    x_far(begin, 0)
    row_in(0)
    with jax.named_scope("x1"):
        x_near_in(1)
    x_far(begin, 1)
    row_in(1)
    row_in(2)

    with jax.named_scope("x2"):
        x_near_in(2)
    x_far(begin, 2)

    heavy = place // 2

    def a_begin(which):
        for d in range(2):

            @pl.when(which == d)
            def _():
                for i in range(3):
                    a_ring(d, i, place).start()

    a_begin(heavy)

    @pl.loop(0, NG)
    def _(g):
        y_step(place, g)

    y_near(0)
    a_begin(1 - heavy)

    @pl.loop(1, NG)
    def _(g):
        y_near(g)

    with jax.named_scope("xfar"):
        for g in range(NG):
            x_far_in(g)

    @pl.loop(0, NG)
    def _(g):
        y_step(across, g)

    @pl.loop(0, NG)
    def _(m):
        rows = pl.ds(pl.multiple_of(m * G, G), G)
        hi, lo = split(xo[rows, :])
        yh[rows, :] = hi
        yl[rows, :] = lo

    left, right = (place + 4 - sign) % 4, (place + 4 + sign) % 4

    def to_partner(q, u):
        return remote(part.at[q, u], precv.at[q, u], ps.at[q, u], pr.at[q, u], {"col": partner})

    def to_other(u):
        return remote(part.at[3, u], pzrecv.at[u], zs.at[u], zr.at[u], {"col": other})

    def role(s):
        j = block_of(s)
        q = (j // 2 + c // 2) % 2
        return q, (j + c) % 2 == 0

    def partial(s, u):
        with jax.named_scope("p"):
            for k in range(2):
                split_unit(acol, s[k], u[k], k)
            value = dot3(yh[...], yl[...], ch[...], cl[...], NT)
            for k in range(2):
                q, mine = role(s[k])
                part[q + 2 * mine.astype(jnp.int32), u[k]] = value[:, k * H : (k + 1) * H]

    def hand_over(s, u):
        for k in range(2):
            q, mine = role(s[k])

            @pl.when(jnp.logical_not(mine))
            def _():
                to_partner(q, u[k]).start()

    def collect(s, u):
        for k in range(2):
            q, mine = role(s[k])

            @pl.when(mine)
            def _():
                with jax.named_scope("pwait"):
                    to_partner(q, u[k]).wait_recv()
                part[2 + q, u[k]] += precv[q, u[k]]

                @pl.when(q == 1)
                def _():
                    to_other(u[k]).start()

    def square(s, u):
        with jax.named_scope("a2"):
            split_units(acol, s, u)
            add_product(a2, block_of(s), u)

    def arrive(i):
        with jax.named_scope("ring"):
            arrived(a_in(i))

    def stage(s, u, meanwhile):
        partial(s, u)
        hand_over(s, u)
        square(*meanwhile)
        collect(s, u)

    own = (place, place)
    for u in range(3):
        partial(own, (u, u + 3))
        hand_over(own, (u, u + 3))
    square(place, (0, 1))
    for u in range(3):
        collect(own, (u, u + 3))

    sides, far_side = (left, right), (across, across)
    arrive(0)
    start(a_out(6))
    stage(sides, (0, 3), (place, (2, 3)))
    arrive(1)
    start(a_out(7))
    stage(sides, (1, 4), (place, (4, 5)))
    arrive(2)
    for i in (8, 3, 4, 5):
        start(a_out(i))
    stage(sides, (2, 5), (left, (0, 1)))
    arrive(6)
    stage(far_side, (0, 3), (right, (3, 4)))
    arrive(7)
    stage(far_side, (1, 4), (across, (0, 3)))
    arrive(8)
    stage(far_side, (2, 5), (across, (1, 4)))
    arrive(3)
    stage(sides, (3, 0), (across, (2, 5)))
    square(left, (2, 3))
    arrive(4)
    stage(sides, (4, 1), (right, (5, 0)))
    arrive(5)
    stage(sides, (5, 2), (left, (4, 5)))
    square(right, (1, 2))

    for u in (0, 3, 1, 4, 2, 5):
        with jax.named_scope("z"):
            to_other(u).wait_recv()
        lanes = slice(u * H, (u + 1) * H)
        xo[:, lanes] = xcol[place, :, lanes] + (part[2, u] + pzrecv[u])

    def sent(copy):
        copy.wait_send()

    for g in range(NG):
        x_near(sent, g)
        x_far(sent, g)
        row_other(g).wait_send()
        row_forward(g).wait_send()

    for i in range(9):
        for copy in a_out(i):
            copy.wait_send()

    for u in range(NU):
        to_partner(0, u).wait_send()
        to_partner(1, u).wait_send()
        to_other(u).wait_send()

    @pl.when(jnp.logical_or(place == 1, place == 2))
    def _():
        for g in range(NG):
            mate(g).wait_send()

    row_partner.wait_send()


def solution(mesh):
    def body(a, x):
        block = pltpu.VMEM((N, N), F32)
        dma = pltpu.SemaphoreType.DMA
        xo, a2 = pl.pallas_call(
            kernel,
            out_shape=(block, block),
            in_specs=[pl.BlockSpec(memory_space=pl.ANY)] * 2,
            out_specs=[pl.BlockSpec(memory_space=pltpu.VMEM)] * 2,
            scratch_shapes=[
                pltpu.VMEM((4, N, N), F32),
                pltpu.VMEM((4, N, N), F32),
                pltpu.VMEM((3, N, N), F32),
                pltpu.VMEM((4, NU, N, H), BF),
                pltpu.VMEM((4, NU, N, H), BF),
                pltpu.VMEM((N, N), BF),
                pltpu.VMEM((N, N), BF),
                pltpu.VMEM((G, N), BF),
                pltpu.VMEM((G, N), BF),
                pltpu.VMEM((4, NU, N, H), F32),
                pltpu.VMEM((2, NU, N, H), F32),
                pltpu.VMEM((NU, N, H), F32),
                dma((2,)),
                dma((2, 2, NG)),
                dma((2, 2, NG)),
                dma((2, 9)),
                dma((2, 9)),
                dma((NG,)),
                dma((NG,)),
                dma((7,)),
                dma((7,)),
                dma((2, NU)),
                dma((2, NU)),
                dma((NU,)),
                dma((NU,)),
            ],
            compiler_params=pltpu.CompilerParams(
                collective_id=0, has_side_effects=True, vmem_limit_bytes=57 * 2**20
            ),
            cost_estimate=pl.CostEstimate(flops=32614907904, bytes_accessed=9437184, transcendentals=0),
        )(a, x)
        return xo, a2

    spec = P(("eq", "row"), "col")
    return jax.shard_map(
        body, mesh=mesh, in_specs=(spec, spec), out_specs=(spec, spec), check_vma=False
    )
```

```python
import jax
import jax.numpy as jnp
from jax import lax
from jax.experimental import pallas as pl
from jax.experimental.pallas import tpu as pltpu
from jax.sharding import PartitionSpec as P

N = 768
G = 256
NG = N // G
H = G // 2
NU = 2 * NG
BF = jnp.bfloat16
F32 = jnp.float32


def split(x):
    hi = x.astype(BF)
    lo = (x - hi.astype(F32)).astype(BF)
    return hi, lo


def dot(a, b, contract):
    return lax.dot_general(a, b, (contract, ((), ())), preferred_element_type=F32)


def dot3(ah, al, bh, bl, contract):
    return dot(ah, bh, contract) + (dot(ah, bl, contract) + dot(al, bh, contract))


NN = ((1,), (0,))
NT = ((1,), (1,))


def kernel(
    a_hbm,
    x_hbm,
    xo,
    a2,
    xcol,
    acol,
    arow,
    arh,
    arl,
    yh,
    yl,
    ch,
    cl,
    part,
    precv,
    pzrecv,
    zx,
    lsem,
    rs,
    rr,
    ns,
    nr,
    ms,
    mr,
    cs,
    cr,
    ws,
    wr,
    ps,
    pr,
    zs,
    zr,
):
    y = lax.axis_index("row")
    c = lax.axis_index("col")
    partner = c + 1 - 2 * (c % 2)
    other = (c + 2) % 4
    other_partner = (partner + 2) % 4

    sign = 1 - 2 * (c % 2)
    place = ((y - c) * sign + 4) % 4
    load_a = pltpu.make_async_copy(a_hbm, acol.at[place], lsem.at[0])
    load_x = pltpu.make_async_copy(x_hbm, xcol.at[place], lsem.at[1])
    load_x.start()
    load_a.start()

    barrier = pltpu.get_barrier_semaphore()
    for where in ({"row": (y + 1) % 4}, {"row": (y + 3) % 4}, {"col": partner}, {"col": other}, {"col": other_partner}):
        pl.semaphore_signal(barrier, inc=1, device_id=where, device_id_type=pl.DeviceIdType.MESH)
    pl.semaphore_wait(barrier, 5)

    def remote(src, dst, send, recv, where):
        return pltpu.make_async_remote_copy(
            src_ref=src,
            dst_ref=dst,
            send_sem=send,
            recv_sem=recv,
            device_id=where,
            device_id_type=pl.DeviceIdType.MESH,
        )

    fwd, bwd = (y + sign + 4) % 4, (y - sign + 4) % 4
    before, after, across = (place + 3) % 4, (place + 1) % 4, (place + 2) % 4

    def ring(d, kind, g, slot, half):
        r0, size = (g * G, G) if half is None else (g * G + half * H, H)
        part = xcol.at[slot, pl.ds(r0, size), pl.ds(0, (g + 1) * G if slot == 0 else N)]
        return remote(part, part, rs.at[d, kind, g], rr.at[d, kind, g], {"row": fwd if d == 0 else bwd})

    def near_of(p, g):
        go = []
        if p != 3 or g > 0:
            go.append((0, 0, g, p, None))
        if p != 1:
            go.append((1, 0, g, p, None))
        return go

    def far_of(p, g):
        if p == 0:
            return ((), ((0, 1, g, 3, 0),), ((0, 1, g, 3, None),))[g]
        if p == 1:
            return ((0, 1, g, 0, 0 if g == 2 else None), (1, 1, g, 2, None))
        if p == 2:
            return (((1, 1, g, 3, None),), ((1, 1, g, 3, 1),), ())[g]
        return ((1, 1, g, 0, 1),) if g == 2 else ()

    def into(table, p, g):
        return [t for t in table((p + 3) % 4, g) if t[0] == 0] + [
            t for t in table((p + 1) % 4, g) if t[0] == 1
        ]

    def each_place(f):
        for p in range(4):

            @pl.when(place == p)
            def _():
                f(p)

    def a_ring(d, i, slot):
        half = (d + c + (1 if 3 <= i < 6 else 0)) % 2
        rows = acol.at[slot, pl.ds(pl.multiple_of(half * (NG * H), H) + (i % 3) * H, H)]
        return remote(rows, rows, ns.at[d, i], nr.at[d, i], {"row": fwd if d == 0 else bwd})

    def a_out(i):
        slots = (before, after) if i >= 6 else (place, place)
        return [a_ring(d, i, slots[d]) for d in range(2)]

    def a_in(i):
        slots = (across, across) if i >= 6 else (before, after)
        return [a_ring(d, i, slots[d]) for d in range(2)]

    def both(make, g):
        return [make(d, g) for d in range(2)]

    def start(copies):
        for copy in copies:
            copy.start()

    def arrived(copies):
        for copy in copies:
            copy.wait_recv()

    def mate(g):
        rows = pl.ds(g * G, G)
        return remote(xcol.at[1, rows], xcol.at[1, rows], ms.at[g], mr.at[g], {"col": partner})

    def corner():
        return remote(xcol.at[3, :, pl.ds(0, G)], zx, cs.at[0], cr.at[0], {"col": other_partner})

    def x_near(act, g):
        each_place(lambda p: [act(ring(*t)) for t in near_of(p, g)])

    def x_far(act, g):
        each_place(lambda p: [act(ring(*t)) for t in far_of(p, g)])

    def x_near_in(g):
        def land(p):
            for t in into(near_of, p, g):
                ring(*t).wait_recv()
            if p == 0:
                mate(g).wait_recv()
            if p == 2:
                mate(g).start()

        each_place(land)

    def x_far_in(g):
        def land(p):
            for t in into(far_of, p, g):
                ring(*t).wait_recv()
            if p == 3:
                mate(g).wait_recv()

        each_place(land)

    def mirror():
        for g, h in ((0, 1), (0, 2), (1, 2)):
            xcol[0, g * G : (g + 1) * G, h * G : (h + 1) * G] = xcol[
                0, h * G : (h + 1) * G, g * G : (g + 1) * G
            ].T

    def begin(copy):
        copy.start()

    row_partner = remote(acol.at[place], arow.at[0], ws.at[0], wr.at[0], {"col": partner})

    def row_other(g):
        rows = pl.ds(g * G, G)
        return remote(acol.at[place, rows], arow.at[1, rows], ws.at[1 + g], wr.at[1 + g], {"col": other})

    def row_forward(g):
        rows = pl.ds(g * G, G)
        return remote(arow.at[1, rows], arow.at[2, rows], ws.at[4 + g], wr.at[4 + g], {"col": partner})

    load_x.wait()
    for g in range(NG):
        x_near(begin, g)

    @pl.when(place == 1)
    def _():
        for g in range(NG):
            mate(g).start()

    load_a.wait()
    for g in range(NG):
        row_other(g).start()
    row_partner.start()

    @pl.when(place == 3)
    def _():
        corner().start()


    def convert(ref, r0, j):
        hi, lo = split(ref[pl.ds(r0, G), :])
        for k in range(NU):
            arh[j, k, pl.ds(r0, G), :] = hi[:, k * H : (k + 1) * H]
            arl[j, k, pl.ds(r0, G), :] = lo[:, k * H : (k + 1) * H]

    @pl.loop(0, NG)
    def _(g):
        convert(acol.at[place], pl.multiple_of(g * G, G), c)

    row_partner.wait_recv()

    @pl.loop(0, NG)
    def _(g):
        convert(arow.at[0], pl.multiple_of(g * G, G), partner)

    def block_of(s):
        return (c + sign * s + 4) % 4

    def pair(ref, j, u):
        return jnp.concatenate([ref[j, u[0]], ref[j, u[1]]], axis=1)

    def split_unit(ref, s, u, at):
        hi, lo = split(ref[s, pl.ds(pl.multiple_of(u * H, H), H), :])
        ch[at * H : (at + 1) * H, :] = hi
        cl[at * H : (at + 1) * H, :] = lo

    def split_units(ref, s, u):
        split_unit(ref, s, u[0], 0)
        split_unit(ref, s, u[1], 1)

    def lanes_of(n):
        return pl.ds(pl.multiple_of(n * G, G), G)

    def add_product(out, j, u):
        @pl.loop(0, NG)
        def _(n):
            lanes = lanes_of(n)
            out[:, lanes] += dot3(pair(arh, j, u), pair(arl, j, u), ch[:, lanes], cl[:, lanes], NN)

    def y_step(s, g):
        with jax.named_scope("y"):
            u = (2 * g, 2 * g + 1)
            split_units(xcol, s, u)
            flipped = jnp.logical_and(s == 1, place % 3 == 0)
            j = block_of(s)

            @pl.when(jnp.logical_not(flipped))
            def _():
                add_product(xo, j, u)

            @pl.when(flipped)
            def _():
                @pl.loop(0, NG)
                def _(k):
                    v = (2 * k, 2 * k + 1)
                    lanes = lanes_of(k)
                    xo[:, lanes_of(g)] += dot3(pair(arh, j, v), pair(arl, j, v), ch[:, lanes], cl[:, lanes], NT)

    def y_near(g):
        @pl.loop(0, 2)
        def _(n):
            y_step((place + 3 + 2 * n) % 4, g)

    def row_in(g):
        with jax.named_scope("row"):
            row_other(g).wait_recv()
            row_forward(g).start()
            convert(arow.at[1], g * G, other)
            row_forward(g).wait_recv()
            convert(arow.at[2], g * G, other_partner)

    xo[...] = jnp.zeros_like(xo)
    a2[...] = jnp.zeros_like(a2)

    with jax.named_scope("x0"):
        x_near_in(0)
    x_far(begin, 0)
    row_in(0)
    with jax.named_scope("x1"):
        x_near_in(1)
    x_far(begin, 1)
    row_in(1)
    with jax.named_scope("x2"):
        x_near_in(2)
    x_far(begin, 2)
    row_in(2)

    def a_begin(late):
        for d, p in ((0, 3), (1, 0)):

            @pl.when((place == p) == late)
            def _():
                for i in range(3):
                    a_ring(d, i, place).start()

    a_begin(False)

    @pl.when(place % 2 == 1)
    def _():
        mirror()

    @pl.loop(0, NG)
    def _(g):
        y_step(place, g)

    a_begin(True)

    @pl.loop(1, NG)
    def _(g):
        y_near(g)

    with jax.named_scope("xfar"):
        for g in range(NG):
            x_far_in(g)

        @pl.when(place == 2)
        def _():
            mirror()

        @pl.when(place == 0)
        def _():
            corner().wait_recv()
            xcol[3, :G, :] = zx[...].T

    y_near(0)

    @pl.loop(0, NG)
    def _(g):
        y_step(across, g)

    @pl.loop(0, NG)
    def _(m):
        rows = pl.ds(pl.multiple_of(m * G, G), G)
        hi, lo = split(xo[rows, :])
        yh[rows, :] = hi
        yl[rows, :] = lo

    left, right = (place + 4 - sign) % 4, (place + 4 + sign) % 4

    def to_partner(q, u):
        return remote(part.at[q, u], precv.at[q, u], ps.at[q, u], pr.at[q, u], {"col": partner})

    def to_other(u):
        return remote(part.at[3, u], pzrecv.at[u], zs.at[u], zr.at[u], {"col": other})

    def role(s):
        j = block_of(s)
        q = (j // 2 + c // 2) % 2
        return q, (j + c) % 2 == 0

    def partial(s, u):
        with jax.named_scope("p"):
            for k in range(2):
                split_unit(acol, s[k], u[k], k)
            value = dot3(yh[...], yl[...], ch[...], cl[...], NT)
            for k in range(2):
                q, mine = role(s[k])
                part[q + 2 * mine.astype(jnp.int32), u[k]] = value[:, k * H : (k + 1) * H]

    def hand_over(s, u):
        for k in range(2):
            q, mine = role(s[k])

            @pl.when(jnp.logical_not(mine))
            def _():
                to_partner(q, u[k]).start()

    def collect(s, u):
        for k in range(2):
            q, mine = role(s[k])

            @pl.when(mine)
            def _():
                with jax.named_scope("pwait"):
                    to_partner(q, u[k]).wait_recv()
                part[2 + q, u[k]] += precv[q, u[k]]

                @pl.when(q == 1)
                def _():
                    to_other(u[k]).start()

    def square(s, u):
        with jax.named_scope("a2"):
            split_units(acol, s, u)
            add_product(a2, block_of(s), u)

    def arrive(i):
        with jax.named_scope("ring"):
            arrived(a_in(i))

    def stage(s, u, meanwhile):
        partial(s, u)
        hand_over(s, u)
        square(*meanwhile)
        collect(s, u)

    arrive(0)
    start(a_out(6))
    own = (place, place)
    for u in range(3):
        partial(own, (u, u + 3))
        hand_over(own, (u, u + 3))
    square(place, (0, 1))
    for u in range(3):
        collect(own, (u, u + 3))

    sides, far_side = (left, right), (across, across)
    stage(sides, (0, 3), (place, (2, 3)))
    arrive(1)
    start(a_out(7))
    stage(sides, (1, 4), (place, (4, 5)))
    arrive(2)
    for i in (8, 3, 4, 5):
        start(a_out(i))
    stage(sides, (2, 5), (left, (0, 1)))
    arrive(6)
    stage(far_side, (0, 3), (right, (3, 4)))
    arrive(7)
    stage(far_side, (1, 4), (across, (0, 3)))
    arrive(8)
    stage(far_side, (2, 5), (across, (1, 4)))
    arrive(3)
    stage(sides, (3, 0), (across, (2, 5)))
    square(left, (2, 3))
    arrive(4)
    stage(sides, (4, 1), (right, (5, 0)))
    arrive(5)
    stage(sides, (5, 2), (left, (4, 5)))
    square(right, (1, 2))

    for u in (0, 3, 1, 4, 2, 5):
        with jax.named_scope("z"):
            to_other(u).wait_recv()
        lanes = slice(u * H, (u + 1) * H)
        xo[:, lanes] = xcol[place, :, lanes] + (part[2, u] + pzrecv[u])

    def sent(copy):
        copy.wait_send()

    for g in range(NG):
        x_near(sent, g)
        x_far(sent, g)
        row_other(g).wait_send()
        row_forward(g).wait_send()

    for i in range(9):
        for copy in a_out(i):
            copy.wait_send()

    for u in range(NU):
        to_partner(0, u).wait_send()
        to_partner(1, u).wait_send()
        to_other(u).wait_send()

    @pl.when(jnp.logical_or(place == 1, place == 2))
    def _():
        for g in range(NG):
            mate(g).wait_send()

    @pl.when(place == 3)
    def _():
        corner().wait_send()

    row_partner.wait_send()


def solution(mesh):
    def body(a, x):
        block = pltpu.VMEM((N, N), F32)
        dma = pltpu.SemaphoreType.DMA
        xo, a2 = pl.pallas_call(
            kernel,
            out_shape=(block, block),
            in_specs=[pl.BlockSpec(memory_space=pl.ANY)] * 2,
            out_specs=[pl.BlockSpec(memory_space=pltpu.VMEM)] * 2,
            scratch_shapes=[
                pltpu.VMEM((4, N, N), F32),
                pltpu.VMEM((4, N, N), F32),
                pltpu.VMEM((3, N, N), F32),
                pltpu.VMEM((4, NU, N, H), BF),
                pltpu.VMEM((4, NU, N, H), BF),
                pltpu.VMEM((N, N), BF),
                pltpu.VMEM((N, N), BF),
                pltpu.VMEM((G, N), BF),
                pltpu.VMEM((G, N), BF),
                pltpu.VMEM((4, NU, N, H), F32),
                pltpu.VMEM((2, NU, N, H), F32),
                pltpu.VMEM((NU, N, H), F32),
                pltpu.VMEM((N, G), F32),
                dma((2,)),
                dma((2, 2, NG)),
                dma((2, 2, NG)),
                dma((2, 9)),
                dma((2, 9)),
                dma((NG,)),
                dma((NG,)),
                dma((1,)),
                dma((1,)),
                dma((7,)),
                dma((7,)),
                dma((2, NU)),
                dma((2, NU)),
                dma((NU,)),
                dma((NU,)),
            ],
            compiler_params=pltpu.CompilerParams(
                collective_id=0, has_side_effects=True, vmem_limit_bytes=57 * 2**20
            ),
            cost_estimate=pl.CostEstimate(flops=32614907904, bytes_accessed=9437184, transcendentals=0),
        )(a, x)
        return xo, a2

    spec = P(("eq", "row"), "col")
    return jax.shard_map(
        body, mesh=mesh, in_specs=(spec, spec), out_specs=(spec, spec), check_vma=False
    )
```

```python
import jax
import jax.numpy as jnp
from jax import lax
from jax.experimental import pallas as pl
from jax.experimental.pallas import tpu as pltpu
from jax.sharding import PartitionSpec as P

N = 768
G = 256
NG = N // G
H = G // 2
NU = 2 * NG
BF = jnp.bfloat16
F32 = jnp.float32


def split(x):
    hi = x.astype(BF)
    lo = (x - hi.astype(F32)).astype(BF)
    return hi, lo


def dot(a, b, contract):
    return lax.dot_general(a, b, (contract, ((), ())), preferred_element_type=F32)


def dot3(ah, al, bh, bl, contract):
    return dot(ah, bh, contract) + (dot(ah, bl, contract) + dot(al, bh, contract))


NN = ((1,), (0,))
NT = ((1,), (1,))


def kernel(
    a_hbm,
    x_hbm,
    xo,
    a2,
    xcol,
    acol,
    arow,
    arh,
    arl,
    yh,
    yl,
    ch,
    cl,
    part,
    precv,
    pzrecv,
    zx,
    lsem,
    rs,
    rr,
    ns,
    nr,
    ms,
    mr,
    cs,
    cr,
    ws,
    wr,
    ps,
    pr,
    zs,
    zr,
):
    y = lax.axis_index("row")
    c = lax.axis_index("col")
    partner = c + 1 - 2 * (c % 2)
    other = (c + 2) % 4
    other_partner = (partner + 2) % 4

    sign = 1 - 2 * (c % 2)
    place = ((y - c) * sign + 4) % 4
    load_a = pltpu.make_async_copy(a_hbm, acol.at[place], lsem.at[0])
    load_x = pltpu.make_async_copy(x_hbm, xcol.at[place], lsem.at[1])
    load_x.start()
    load_a.start()

    barrier = pltpu.get_barrier_semaphore()
    for where in ({"row": (y + 1) % 4}, {"row": (y + 3) % 4}, {"col": partner}, {"col": other}, {"col": other_partner}):
        pl.semaphore_signal(barrier, inc=1, device_id=where, device_id_type=pl.DeviceIdType.MESH)
    pl.semaphore_wait(barrier, 5)

    def remote(src, dst, send, recv, where):
        return pltpu.make_async_remote_copy(
            src_ref=src,
            dst_ref=dst,
            send_sem=send,
            recv_sem=recv,
            device_id=where,
            device_id_type=pl.DeviceIdType.MESH,
        )

    fwd, bwd = (y + sign + 4) % 4, (y - sign + 4) % 4
    before, after, across = (place + 3) % 4, (place + 1) % 4, (place + 2) % 4

    def ring(d, kind, g, slot, half):
        r0, size = (g * G, G) if half is None else (g * G + half * H, H)
        part = xcol.at[slot, pl.ds(r0, size), pl.ds(0, (g + 1) * G if slot == 0 else N)]
        return remote(part, part, rs.at[d, kind, g], rr.at[d, kind, g], {"row": fwd if d == 0 else bwd})

    def near_of(p, g):
        go = []
        if p != 3 or g > 0:
            go.append((0, 0, g, p, None))
        if p != 1:
            go.append((1, 0, g, p, None))
        return go

    def far_of(p, g):
        if p == 0:
            return ((), ((0, 1, g, 3, 0),), ((0, 1, g, 3, None),))[g]
        if p == 1:
            return ((0, 1, g, 0, 0 if g == 2 else None), (1, 1, g, 2, None))
        if p == 2:
            return (((1, 1, g, 3, None),), ((1, 1, g, 3, 1),), ())[g]
        return ((1, 1, g, 0, 1),) if g == 2 else ()

    def into(table, p, g):
        return [t for t in table((p + 3) % 4, g) if t[0] == 0] + [
            t for t in table((p + 1) % 4, g) if t[0] == 1
        ]

    def each_place(f):
        for p in range(4):

            @pl.when(place == p)
            def _():
                f(p)

    def a_ring(d, i, slot):
        half = (d + c + (1 if 3 <= i < 6 else 0)) % 2
        rows = acol.at[slot, pl.ds(pl.multiple_of(half * (NG * H), H) + (i % 3) * H, H)]
        return remote(rows, rows, ns.at[d, i], nr.at[d, i], {"row": fwd if d == 0 else bwd})

    def a_out(i):
        slots = (before, after) if i >= 6 else (place, place)
        return [a_ring(d, i, slots[d]) for d in range(2)]

    def a_in(i):
        slots = (across, across) if i >= 6 else (before, after)
        return [a_ring(d, i, slots[d]) for d in range(2)]

    def both(make, g):
        return [make(d, g) for d in range(2)]

    def start(copies):
        for copy in copies:
            copy.start()

    def arrived(copies):
        for copy in copies:
            copy.wait_recv()

    def mate(g):
        rows = pl.ds(g * G, G)
        return remote(xcol.at[1, rows], xcol.at[1, rows], ms.at[g], mr.at[g], {"col": partner})

    def corner():
        return remote(xcol.at[3, :, pl.ds(0, G)], zx, cs.at[0], cr.at[0], {"col": other_partner})

    def x_near(act, g):
        each_place(lambda p: [act(ring(*t)) for t in near_of(p, g)])

    def x_far(act, g):
        each_place(lambda p: [act(ring(*t)) for t in far_of(p, g)])

    def x_near_in(g):
        def land(p):
            for t in into(near_of, p, g):
                ring(*t).wait_recv()
            if p == 0:
                mate(g).wait_recv()
            if p == 2:
                mate(g).start()

        each_place(land)

    def x_far_in(g):
        def land(p):
            for t in into(far_of, p, g):
                ring(*t).wait_recv()
            if p == 3:
                mate(g).wait_recv()

        each_place(land)

    def mirror():
        for g, h in ((0, 1), (0, 2), (1, 2)):
            xcol[0, g * G : (g + 1) * G, h * G : (h + 1) * G] = xcol[
                0, h * G : (h + 1) * G, g * G : (g + 1) * G
            ].T

    def begin(copy):
        copy.start()

    row_partner = remote(acol.at[place], arow.at[0], ws.at[0], wr.at[0], {"col": partner})

    def a_begin(d, units, where):
        for p in where:

            @pl.when(place == p)
            def _():
                for i in units:
                    a_ring(d, i, p).start()

    def row_other(g):
        rows = pl.ds(g * G, G)
        return remote(acol.at[place, rows], arow.at[1, rows], ws.at[1 + g], wr.at[1 + g], {"col": other})

    def row_forward(g):
        rows = pl.ds(g * G, G)
        return remote(arow.at[1, rows], arow.at[2, rows], ws.at[4 + g], wr.at[4 + g], {"col": partner})

    load_x.wait()
    for g in range(NG):
        x_near(begin, g)

    @pl.when(place == 1)
    def _():
        for g in range(NG):
            mate(g).start()

    load_a.wait()
    for g in range(NG):
        row_other(g).start()
    row_partner.start()

    a_begin(0, (0, 1, 2), (0,))

    @pl.when(place == 3)
    def _():
        corner().start()


    def convert(ref, r0, j):
        hi, lo = split(ref[pl.ds(r0, G), :])
        for k in range(NU):
            arh[j, k, pl.ds(r0, G), :] = hi[:, k * H : (k + 1) * H]
            arl[j, k, pl.ds(r0, G), :] = lo[:, k * H : (k + 1) * H]

    @pl.loop(0, NG)
    def _(g):
        convert(acol.at[place], pl.multiple_of(g * G, G), c)

    row_partner.wait_recv()

    @pl.loop(0, NG)
    def _(g):
        convert(arow.at[0], pl.multiple_of(g * G, G), partner)

    def block_of(s):
        return (c + sign * s + 4) % 4

    def pair(ref, j, u):
        return jnp.concatenate([ref[j, u[0]], ref[j, u[1]]], axis=1)

    def split_unit(ref, s, u, at):
        hi, lo = split(ref[s, pl.ds(pl.multiple_of(u * H, H), H), :])
        ch[at * H : (at + 1) * H, :] = hi
        cl[at * H : (at + 1) * H, :] = lo

    def split_units(ref, s, u):
        split_unit(ref, s, u[0], 0)
        split_unit(ref, s, u[1], 1)

    def lanes_of(n):
        return pl.ds(pl.multiple_of(n * G, G), G)

    def add_product(out, j, u, unroll=False):
        @pl.loop(0, NG, unroll=unroll)
        def _(n):
            lanes = lanes_of(n)
            out[:, lanes] += dot3(pair(arh, j, u), pair(arl, j, u), ch[:, lanes], cl[:, lanes], NN)

    def y_step(s, g):
        with jax.named_scope("y"):
            u = (2 * g, 2 * g + 1)
            split_units(xcol, s, u)
            flipped = jnp.logical_and(s == 1, place % 3 == 0)
            j = block_of(s)

            @pl.when(jnp.logical_not(flipped))
            def _():
                add_product(xo, j, u, True)

            @pl.when(flipped)
            def _():
                @pl.loop(0, NG)
                def _(k):
                    v = (2 * k, 2 * k + 1)
                    lanes = lanes_of(k)
                    xo[:, lanes_of(g)] += dot3(pair(arh, j, v), pair(arl, j, v), ch[:, lanes], cl[:, lanes], NT)

    def y_near(g):
        @pl.loop(0, 2)
        def _(n):
            y_step((place + 3 + 2 * n) % 4, g)

    def arrive(i):
        with jax.named_scope("ring"):
            arrived(a_in(i))

    def row_in(g):
        with jax.named_scope("row"):
            row_other(g).wait_recv()
            row_forward(g).start()
            convert(arow.at[1], g * G, other)
            row_forward(g).wait_recv()
            convert(arow.at[2], g * G, other_partner)

    xo[...] = jnp.zeros_like(xo)
    a2[...] = jnp.zeros_like(a2)

    with jax.named_scope("x0"):
        x_near_in(0)
    x_far(begin, 0)
    row_in(0)
    with jax.named_scope("x1"):
        x_near_in(1)
    x_far(begin, 1)
    a_begin(0, (0,), (1, 2))
    a_begin(1, (0,), (2, 3))
    row_in(1)
    with jax.named_scope("x2"):
        x_near_in(2)
    x_far(begin, 2)

    a_begin(0, (1, 2), (1, 2))
    a_begin(1, (0, 1, 2), (1,))
    a_begin(1, (1, 2), (2, 3))
    a_begin(1, (0,), (0,))
    row_in(2)
    a_begin(0, (0, 1, 2), (3,))
    a_begin(1, (1, 2), (0,))

    @pl.when(place % 2 == 1)
    def _():
        mirror()

    @pl.loop(0, NG)
    def _(g):
        y_step(place, g)

    @pl.loop(1, NG)
    def _(g):
        y_near(g)

    with jax.named_scope("xfar"):
        for g in range(NG):
            x_far_in(g)

        @pl.when(place == 2)
        def _():
            mirror()

        @pl.when(place == 0)
        def _():
            corner().wait_recv()
            xcol[3, :G, :] = zx[...].T

    y_near(0)
    arrive(0)
    start(a_out(6))

    @pl.loop(0, NG)
    def _(g):
        y_step(across, g)

    @pl.loop(0, NG)
    def _(m):
        rows = pl.ds(pl.multiple_of(m * G, G), G)
        hi, lo = split(xo[rows, :])
        yh[rows, :] = hi
        yl[rows, :] = lo

    left, right = (place + 4 - sign) % 4, (place + 4 + sign) % 4

    def to_partner(q, u):
        return remote(part.at[q, u], precv.at[q, u], ps.at[q, u], pr.at[q, u], {"col": partner})

    def to_other(u):
        return remote(part.at[3, u], pzrecv.at[u], zs.at[u], zr.at[u], {"col": other})

    def role(s):
        j = block_of(s)
        q = (j // 2 + c // 2) % 2
        return q, (j + c) % 2 == 0

    def partial(s, u):
        with jax.named_scope("p"):
            for k in range(2):
                split_unit(acol, s[k], u[k], k)
            value = dot3(yh[...], yl[...], ch[...], cl[...], NT)
            for k in range(2):
                q, mine = role(s[k])
                part[q + 2 * mine.astype(jnp.int32), u[k]] = value[:, k * H : (k + 1) * H]

    def hand_over(s, u):
        for k in range(2):
            q, mine = role(s[k])

            @pl.when(jnp.logical_not(mine))
            def _():
                to_partner(q, u[k]).start()

    def collect(s, u):
        for k in range(2):
            q, mine = role(s[k])

            @pl.when(mine)
            def _():
                with jax.named_scope("pwait"):
                    to_partner(q, u[k]).wait_recv()
                part[2 + q, u[k]] += precv[q, u[k]]

                @pl.when(q == 1)
                def _():
                    to_other(u[k]).start()

    def square(s, u):
        with jax.named_scope("a2"):
            split_units(acol, s, u)
            add_product(a2, block_of(s), u)

    def sums(s, u):
        partial(s, u)
        hand_over(s, u)

    def stage(s, u, meanwhile):
        sums(s, u)
        square(*meanwhile)
        collect(s, u)

    own, sides, far_side = (place, place), (left, right), (across, across)
    arrive(1)
    start(a_out(7))
    sums(sides, (0, 3))
    sums(sides, (1, 4))
    collect(sides, (0, 3))
    arrive(2)
    for i in (8, 3, 4, 5):
        start(a_out(i))
    sums(sides, (2, 5))
    collect(sides, (1, 4))
    sums(own, (0, 3))
    collect(sides, (2, 5))
    sums(own, (1, 4))
    collect(own, (0, 3))
    sums(own, (2, 5))
    collect(own, (1, 4))
    arrive(6)
    sums(far_side, (0, 3))
    collect(own, (2, 5))
    square(place, (0, 1))
    collect(far_side, (0, 3))
    square(place, (2, 3))
    arrive(7)
    stage(far_side, (1, 4), (place, (4, 5)))
    square(left, (0, 1))
    arrive(8)
    stage(far_side, (2, 5), (right, (3, 4)))
    square(across, (0, 3))
    arrive(3)
    stage(sides, (3, 0), (across, (1, 4)))
    square(across, (2, 5))
    arrive(4)
    stage(sides, (4, 1), (left, (2, 3)))
    arrive(5)
    stage(sides, (5, 2), (right, (5, 0)))
    square(left, (4, 5))
    square(right, (1, 2))

    for u in (0, 3, 1, 4, 2, 5):
        with jax.named_scope("z"):
            to_other(u).wait_recv()
        lanes = slice(u * H, (u + 1) * H)
        xo[:, lanes] = xcol[place, :, lanes] + (part[2, u] + pzrecv[u])

    def sent(copy):
        copy.wait_send()

    for g in range(NG):
        x_near(sent, g)
        x_far(sent, g)
        row_other(g).wait_send()
        row_forward(g).wait_send()

    for i in range(9):
        for copy in a_out(i):
            copy.wait_send()

    for u in range(NU):
        to_partner(0, u).wait_send()
        to_partner(1, u).wait_send()
        to_other(u).wait_send()

    @pl.when(jnp.logical_or(place == 1, place == 2))
    def _():
        for g in range(NG):
            mate(g).wait_send()

    @pl.when(place == 3)
    def _():
        corner().wait_send()

    row_partner.wait_send()


def solution(mesh):
    def body(a, x):
        block = pltpu.VMEM((N, N), F32)
        dma = pltpu.SemaphoreType.DMA
        xo, a2 = pl.pallas_call(
            kernel,
            out_shape=(block, block),
            in_specs=[pl.BlockSpec(memory_space=pl.ANY)] * 2,
            out_specs=[pl.BlockSpec(memory_space=pltpu.VMEM)] * 2,
            scratch_shapes=[
                pltpu.VMEM((4, N, N), F32),
                pltpu.VMEM((4, N, N), F32),
                pltpu.VMEM((3, N, N), F32),
                pltpu.VMEM((4, NU, N, H), BF),
                pltpu.VMEM((4, NU, N, H), BF),
                pltpu.VMEM((N, N), BF),
                pltpu.VMEM((N, N), BF),
                pltpu.VMEM((G, N), BF),
                pltpu.VMEM((G, N), BF),
                pltpu.VMEM((4, NU, N, H), F32),
                pltpu.VMEM((2, NU, N, H), F32),
                pltpu.VMEM((NU, N, H), F32),
                pltpu.VMEM((N, G), F32),
                dma((2,)),
                dma((2, 2, NG)),
                dma((2, 2, NG)),
                dma((2, 9)),
                dma((2, 9)),
                dma((NG,)),
                dma((NG,)),
                dma((1,)),
                dma((1,)),
                dma((7,)),
                dma((7,)),
                dma((2, NU)),
                dma((2, NU)),
                dma((NU,)),
                dma((NU,)),
            ],
            compiler_params=pltpu.CompilerParams(
                collective_id=0, has_side_effects=True, vmem_limit_bytes=57 * 2**20
            ),
            cost_estimate=pl.CostEstimate(flops=32614907904, bytes_accessed=9437184, transcendentals=0),
        )(a, x)
        return xo, a2

    spec = P(("eq", "row"), "col")
    return jax.shard_map(
        body, mesh=mesh, in_specs=(spec, spec), out_specs=(spec, spec), check_vma=False
    )
```

```python
import jax
import jax.numpy as jnp
from jax import lax
from jax.experimental import pallas as pl
from jax.experimental.pallas import tpu as pltpu
from jax.sharding import PartitionSpec as P

N = 768
G = 256
NG = N // G
H = G // 2
NU = 2 * NG
BF = jnp.bfloat16
F32 = jnp.float32


def split(x):
    hi = x.astype(BF)
    lo = (x - hi.astype(F32)).astype(BF)
    return hi, lo


def dot(a, b, contract):
    return lax.dot_general(a, b, (contract, ((), ())), preferred_element_type=F32)


def dot3(ah, al, bh, bl, contract):
    return dot(ah, bh, contract) + (dot(ah, bl, contract) + dot(al, bh, contract))


NN = ((1,), (0,))
NT = ((1,), (1,))


def kernel(
    a_hbm,
    x_hbm,
    xo,
    a2,
    xcol,
    acol,
    arow,
    arh,
    arl,
    yh,
    yl,
    ch,
    cl,
    part,
    precv,
    pzrecv,
    zx,
    lsem,
    rs,
    rr,
    ns,
    nr,
    ms,
    mr,
    cs,
    cr,
    ws,
    wr,
    ps,
    pr,
    zs,
    zr,
):
    y = lax.axis_index("row")
    c = lax.axis_index("col")
    partner = c + 1 - 2 * (c % 2)
    other = (c + 2) % 4
    other_partner = (partner + 2) % 4

    sign = 1 - 2 * (c % 2)
    place = ((y - c) * sign + 4) % 4
    load_a = pltpu.make_async_copy(a_hbm, acol.at[place], lsem.at[0])
    load_x = pltpu.make_async_copy(x_hbm, xcol.at[place], lsem.at[1])
    load_x.start()
    load_a.start()

    barrier = pltpu.get_barrier_semaphore()
    for where in ({"row": (y + 1) % 4}, {"row": (y + 3) % 4}, {"col": partner}, {"col": other}, {"col": other_partner}):
        pl.semaphore_signal(barrier, inc=1, device_id=where, device_id_type=pl.DeviceIdType.MESH)
    pl.semaphore_wait(barrier, 5)

    def remote(src, dst, send, recv, where):
        return pltpu.make_async_remote_copy(
            src_ref=src,
            dst_ref=dst,
            send_sem=send,
            recv_sem=recv,
            device_id=where,
            device_id_type=pl.DeviceIdType.MESH,
        )

    fwd, bwd = (y + sign + 4) % 4, (y - sign + 4) % 4
    before, after, across = (place + 3) % 4, (place + 1) % 4, (place + 2) % 4

    def ring(d, kind, slot, u, n=2):
        part = xcol.at[slot, pl.ds(u * H, n * H), pl.ds(0, (u + n) * H if slot == 0 else N)]
        return remote(part, part, rs.at[d, kind, u], rr.at[d, kind, u], {"row": fwd if d == 0 else bwd})

    def near_of(p, g):
        u = 2 * g
        if p == 0:
            return [(d, 0, 0, v, 1) for v in (u, u + 1) for d in range(2)]
        if p == 1:
            return [(0, 0, 1, u, 2)]
        if p == 2:
            return [(d, 0, 2, u, 2) for d in range(2)]
        return [(1, 0, 3, u, 2)] + ([], [(0, 0, 3, 3, 1)], [(0, 0, 3, 4, 2)])[g]

    def far_of(p, g):
        u = 2 * g
        if p == 0:
            return ([], [(0, 1, 3, 3, 1)], [(0, 1, 3, 4, 2)])[g]
        if p == 1:
            return [(0, 1, 0, v, 1) for v in (u, u + 1) if v != 2] + [(1, 1, 2, u, 2)]
        if p == 2:
            return ([(1, 1, 3, 0, 2)], [(1, 1, 3, 2, 1)], [])[g]
        return [(1, 1, 0, 2, 1)] if g == 1 else []

    def into(table, p, g):
        return [t for t in table((p + 3) % 4, g) if t[0] == 0] + [
            t for t in table((p + 1) % 4, g) if t[0] == 1
        ]

    def each_place(f):
        for p in range(4):

            @pl.when(place == p)
            def _():
                f(p)

    def a_ring(d, i, slot):
        half = (d + c + (1 if 3 <= i < 6 else 0)) % 2
        rows = acol.at[slot, pl.ds(pl.multiple_of(half * (NG * H), H) + (i % 3) * H, H)]
        return remote(rows, rows, ns.at[d, i], nr.at[d, i], {"row": fwd if d == 0 else bwd})

    def a_out(i):
        slots = (before, after) if i >= 6 else (place, place)
        return [a_ring(d, i, slots[d]) for d in range(2)]

    def a_in(i):
        slots = (across, across) if i >= 6 else (before, after)
        return [a_ring(d, i, slots[d]) for d in range(2)]

    def both(make, g):
        return [make(d, g) for d in range(2)]

    def start(copies):
        for copy in copies:
            copy.start()

    def arrived(copies):
        for copy in copies:
            copy.wait_recv()

    def mate(g):
        rows = pl.ds(g * G, G)
        return remote(xcol.at[1, rows], xcol.at[1, rows], ms.at[g], mr.at[g], {"col": partner})

    def corner():
        return remote(xcol.at[3, :, pl.ds(0, NG * H)], zx, cs.at[0], cr.at[0], {"col": other_partner})

    def x_near(act, g):
        each_place(lambda p: [act(ring(*t)) for t in near_of(p, g)])

    def x_far(act, g):
        each_place(lambda p: [act(ring(*t)) for t in far_of(p, g)])

    def x_near_in(g):
        def land(p):
            for t in into(near_of, p, g):
                ring(*t).wait_recv()
            if p == 0:
                mate(g).wait_recv()
            if p == 2:
                mate(g).start()

        each_place(land)

    def x_far_in(g):
        def land(p):
            for t in into(far_of, p, g):
                ring(*t).wait_recv()
            if p == 3:
                mate(g).wait_recv()

        each_place(land)

    def mirror():
        for u in range(NU - 1):
            v = slice((u + 1) * H, N)
            xcol[0, u * H : (u + 1) * H, v] = xcol[0, v, u * H : (u + 1) * H].T

    def begin(copy):
        copy.start()

    row_partner = remote(acol.at[place], arow.at[0], ws.at[0], wr.at[0], {"col": partner})

    def a_begin(d, units, where):
        for p in where:

            @pl.when(place == p)
            def _():
                for i in units:
                    a_ring(d, i, p).start()

    def row_other(g):
        rows = pl.ds(g * G, G)
        return remote(acol.at[place, rows], arow.at[1, rows], ws.at[1 + g], wr.at[1 + g], {"col": other})

    def row_forward(g):
        rows = pl.ds(g * G, G)
        return remote(arow.at[1, rows], arow.at[2, rows], ws.at[4 + g], wr.at[4 + g], {"col": partner})

    load_x.wait()
    for g in range(NG):
        x_near(begin, g)

    @pl.when(place == 1)
    def _():
        for g in range(NG):
            mate(g).start()

    load_a.wait()
    for g in range(NG):
        row_other(g).start()
    row_partner.start()

    a_begin(0, (0, 1, 2), (0,))


    def convert(ref, r0, j):
        hi, lo = split(ref[pl.ds(r0, G), :])
        for k in range(NU):
            arh[j, k, pl.ds(r0, G), :] = hi[:, k * H : (k + 1) * H]
            arl[j, k, pl.ds(r0, G), :] = lo[:, k * H : (k + 1) * H]

    @pl.loop(0, NG)
    def _(g):
        convert(acol.at[place], pl.multiple_of(g * G, G), c)

    row_partner.wait_recv()

    @pl.loop(0, NG)
    def _(g):
        convert(arow.at[0], pl.multiple_of(g * G, G), partner)

    def block_of(s):
        return (c + sign * s + 4) % 4

    def pair(ref, j, u):
        return jnp.concatenate([ref[j, u[0]], ref[j, u[1]]], axis=1)

    def split_unit(ref, s, u, at):
        hi, lo = split(ref[s, pl.ds(pl.multiple_of(u * H, H), H), :])
        ch[at * H : (at + 1) * H, :] = hi
        cl[at * H : (at + 1) * H, :] = lo

    def split_units(ref, s, u):
        split_unit(ref, s, u[0], 0)
        split_unit(ref, s, u[1], 1)

    def lanes_of(n):
        return pl.ds(pl.multiple_of(n * G, G), G)

    def add_product(out, j, u, unroll=False):
        @pl.loop(0, NG, unroll=unroll)
        def _(n):
            lanes = lanes_of(n)
            out[:, lanes] += dot3(pair(arh, j, u), pair(arl, j, u), ch[:, lanes], cl[:, lanes], NN)

    def y_step(s, g):
        with jax.named_scope("y"):
            u = (2 * g, 2 * g + 1)
            split_units(xcol, s, u)
            flipped = jnp.logical_and(s == 1, place % 3 == 0)
            j = block_of(s)

            @pl.when(jnp.logical_not(flipped))
            def _():
                add_product(xo, j, u, True)

            @pl.when(flipped)
            def _():
                @pl.loop(0, NG)
                def _(k):
                    v = (2 * k, 2 * k + 1)
                    lanes = lanes_of(k)
                    xo[:, lanes_of(g)] += dot3(pair(arh, j, v), pair(arl, j, v), ch[:, lanes], cl[:, lanes], NT)

    def y_near(g):
        @pl.loop(0, 2)
        def _(n):
            y_step((place + 3 + 2 * n) % 4, g)

    def arrive(i):
        with jax.named_scope("ring"):
            arrived(a_in(i))

    def row_in(g):
        with jax.named_scope("row"):
            row_other(g).wait_recv()
            row_forward(g).start()
            convert(arow.at[1], g * G, other)
            row_forward(g).wait_recv()
            convert(arow.at[2], g * G, other_partner)

    xo[...] = jnp.zeros_like(xo)
    a2[...] = jnp.zeros_like(a2)

    with jax.named_scope("x0"):
        x_near_in(0)
    x_far(begin, 0)
    row_in(0)
    with jax.named_scope("x1"):
        x_near_in(1)
    x_far(begin, 1)
    a_begin(0, (0,), (1, 2))
    a_begin(1, (0,), (2, 3))
    row_in(1)
    with jax.named_scope("x2"):
        x_near_in(2)
    x_far(begin, 2)


    @pl.when(place == 3)
    def _():
        corner().start()

    a_begin(0, (1, 2), (1, 2))
    a_begin(1, (0, 1, 2), (1,))
    a_begin(1, (1, 2), (2, 3))
    a_begin(1, (0,), (0,))
    row_in(2)
    a_begin(0, (0, 1, 2), (3,))
    a_begin(1, (1, 2), (0,))

    @pl.when(place % 2 == 1)
    def _():
        mirror()

    @pl.loop(0, NG)
    def _(g):
        y_step(place, g)

    y_near(2)
    with jax.named_scope("xfar"):
        for g in range(NG):
            x_far_in(g)

        @pl.when(place == 2)
        def _():
            mirror()

    @pl.loop(0, NG)
    def _(g):
        y_step(across, g)

    arrive(0)
    start(a_out(6))
    with jax.named_scope("corner"):

        @pl.when(place == 0)
        def _():
            corner().wait_recv()
            xcol[3, : NG * H, :] = zx[...].T

    @pl.loop(0, 2)
    def _(g):
        y_near(g)

    @pl.loop(0, NG)
    def _(m):
        rows = pl.ds(pl.multiple_of(m * G, G), G)
        hi, lo = split(xo[rows, :])
        yh[rows, :] = hi
        yl[rows, :] = lo

    left, right = (place + 4 - sign) % 4, (place + 4 + sign) % 4

    def to_partner(q, u):
        return remote(part.at[q, u], precv.at[q, u], ps.at[q, u], pr.at[q, u], {"col": partner})

    def to_other(u):
        return remote(part.at[3, u], pzrecv.at[u], zs.at[u], zr.at[u], {"col": other})

    def role(s):
        j = block_of(s)
        q = (j // 2 + c // 2) % 2
        return q, (j + c) % 2 == 0

    def partial(s, u):
        with jax.named_scope("p"):
            for k in range(2):
                split_unit(acol, s[k], u[k], k)
            value = dot3(yh[...], yl[...], ch[...], cl[...], NT)
            for k in range(2):
                q, mine = role(s[k])
                part[q + 2 * mine.astype(jnp.int32), u[k]] = value[:, k * H : (k + 1) * H]

    def hand_over(s, u):
        for k in range(2):
            q, mine = role(s[k])

            @pl.when(jnp.logical_not(mine))
            def _():
                to_partner(q, u[k]).start()

    def collect(s, u):
        for k in range(2):
            q, mine = role(s[k])

            @pl.when(mine)
            def _():
                with jax.named_scope("pwait"):
                    to_partner(q, u[k]).wait_recv()
                part[2 + q, u[k]] += precv[q, u[k]]

                @pl.when(q == 1)
                def _():
                    to_other(u[k]).start()

    def square(s, u):
        with jax.named_scope("a2"):
            split_units(acol, s, u)
            add_product(a2, block_of(s), u)

    def sums(s, u):
        partial(s, u)
        hand_over(s, u)

    def stage(s, u, meanwhile):
        sums(s, u)
        square(*meanwhile)
        collect(s, u)

    own, sides, far_side = (place, place), (left, right), (across, across)
    arrive(1)
    start(a_out(7))
    sums(sides, (0, 3))
    sums(sides, (1, 4))
    collect(sides, (0, 3))
    arrive(2)
    for i in (8, 3, 4, 5):
        start(a_out(i))
    sums(sides, (2, 5))
    collect(sides, (1, 4))
    sums(own, (0, 3))
    collect(sides, (2, 5))
    sums(own, (1, 4))
    collect(own, (0, 3))
    sums(own, (2, 5))
    collect(own, (1, 4))
    arrive(6)
    sums(far_side, (0, 3))
    collect(own, (2, 5))
    square(place, (0, 1))
    collect(far_side, (0, 3))
    square(place, (2, 3))
    arrive(7)
    stage(far_side, (1, 4), (place, (4, 5)))
    square(left, (0, 1))
    arrive(8)
    stage(far_side, (2, 5), (right, (3, 4)))
    square(across, (0, 3))
    arrive(3)
    stage(sides, (3, 0), (across, (1, 4)))
    square(across, (2, 5))
    arrive(4)
    stage(sides, (4, 1), (left, (2, 3)))
    arrive(5)
    stage(sides, (5, 2), (right, (5, 0)))
    square(left, (4, 5))
    square(right, (1, 2))

    for u in (0, 3, 1, 4, 2, 5):
        with jax.named_scope("z"):
            to_other(u).wait_recv()
        lanes = slice(u * H, (u + 1) * H)
        xo[:, lanes] = xcol[place, :, lanes] + (part[2, u] + pzrecv[u])

    def sent(copy):
        copy.wait_send()

    for g in range(NG):
        x_near(sent, g)
        x_far(sent, g)
        row_other(g).wait_send()
        row_forward(g).wait_send()

    for i in range(9):
        for copy in a_out(i):
            copy.wait_send()

    for u in range(NU):
        to_partner(0, u).wait_send()
        to_partner(1, u).wait_send()
        to_other(u).wait_send()

    @pl.when(jnp.logical_or(place == 1, place == 2))
    def _():
        for g in range(NG):
            mate(g).wait_send()

    @pl.when(place == 3)
    def _():
        corner().wait_send()

    row_partner.wait_send()


def solution(mesh):
    def body(a, x):
        block = pltpu.VMEM((N, N), F32)
        dma = pltpu.SemaphoreType.DMA
        xo, a2 = pl.pallas_call(
            kernel,
            out_shape=(block, block),
            in_specs=[pl.BlockSpec(memory_space=pl.ANY)] * 2,
            out_specs=[pl.BlockSpec(memory_space=pltpu.VMEM)] * 2,
            scratch_shapes=[
                pltpu.VMEM((4, N, N), F32),
                pltpu.VMEM((4, N, N), F32),
                pltpu.VMEM((3, N, N), F32),
                pltpu.VMEM((4, NU, N, H), BF),
                pltpu.VMEM((4, NU, N, H), BF),
                pltpu.VMEM((N, N), BF),
                pltpu.VMEM((N, N), BF),
                pltpu.VMEM((G, N), BF),
                pltpu.VMEM((G, N), BF),
                pltpu.VMEM((4, NU, N, H), F32),
                pltpu.VMEM((2, NU, N, H), F32),
                pltpu.VMEM((NU, N, H), F32),
                pltpu.VMEM((N, NG * H), F32),
                dma((2,)),
                dma((2, 2, NU)),
                dma((2, 2, NU)),
                dma((2, 9)),
                dma((2, 9)),
                dma((NG,)),
                dma((NG,)),
                dma((1,)),
                dma((1,)),
                dma((7,)),
                dma((7,)),
                dma((2, NU)),
                dma((2, NU)),
                dma((NU,)),
                dma((NU,)),
            ],
            compiler_params=pltpu.CompilerParams(
                collective_id=0, has_side_effects=True, vmem_limit_bytes=57 * 2**20
            ),
            cost_estimate=pl.CostEstimate(flops=32614907904, bytes_accessed=9437184, transcendentals=0),
        )(a, x)
        return xo, a2

    spec = P(("eq", "row"), "col")
    return jax.shard_map(
        body, mesh=mesh, in_specs=(spec, spec), out_specs=(spec, spec), check_vma=False
    )
```

```python
import jax
import jax.numpy as jnp
from jax import lax
from jax.experimental import pallas as pl
from jax.experimental.pallas import tpu as pltpu
from jax.sharding import PartitionSpec as P

N = 768
G = 256
NG = N // G
H = G // 2
NU = 2 * NG
BF = jnp.bfloat16
F32 = jnp.float32


def split(x):
    hi = x.astype(BF)
    lo = (x - hi.astype(F32)).astype(BF)
    return hi, lo


def dot(a, b, contract):
    return lax.dot_general(a, b, (contract, ((), ())), preferred_element_type=F32)


def dot3(ah, al, bh, bl, contract):
    return dot(ah, bh, contract) + (dot(ah, bl, contract) + dot(al, bh, contract))


NN = ((1,), (0,))
NT = ((1,), (1,))


def kernel(
    a_hbm,
    x_hbm,
    xo,
    a2,
    xcol,
    acol,
    arow,
    arh,
    arl,
    yh,
    yl,
    ch,
    cl,
    part,
    precv,
    pzrecv,
    zx,
    lsem,
    rs,
    rr,
    ns,
    nr,
    ms,
    mr,
    cs,
    cr,
    ws,
    wr,
    ps,
    pr,
    zs,
    zr,
    hs,
    hr,
):
    y = lax.axis_index("row")
    c = lax.axis_index("col")
    partner = c + 1 - 2 * (c % 2)
    other = (c + 2) % 4
    other_partner = (partner + 2) % 4

    sign = 1 - 2 * (c % 2)
    place = ((y - c) * sign + 4) % 4
    load_a = pltpu.make_async_copy(a_hbm, acol.at[place], lsem.at[0])
    load_x = pltpu.make_async_copy(x_hbm, xcol.at[place], lsem.at[1])
    load_x.start()
    load_a.start()

    barrier = pltpu.get_barrier_semaphore()
    for where in ({"row": (y + 1) % 4}, {"row": (y + 3) % 4}, {"col": partner}, {"col": other}, {"col": other_partner}):
        pl.semaphore_signal(barrier, inc=1, device_id=where, device_id_type=pl.DeviceIdType.MESH)
    pl.semaphore_wait(barrier, 5)

    def remote(src, dst, send, recv, where):
        return pltpu.make_async_remote_copy(
            src_ref=src,
            dst_ref=dst,
            send_sem=send,
            recv_sem=recv,
            device_id=where,
            device_id_type=pl.DeviceIdType.MESH,
        )

    fwd, bwd = (y + sign + 4) % 4, (y - sign + 4) % 4
    before, after, across = (place + 3) % 4, (place + 1) % 4, (place + 2) % 4

    def ring(d, kind, slot, u, n=2):
        part = xcol.at[slot, pl.ds(u * H, n * H), pl.ds(0, (u + n) * H if slot == 0 else N)]
        return remote(part, part, rs.at[d, kind, u], rr.at[d, kind, u], {"row": fwd if d == 0 else bwd})

    def near_of(p, g):
        u = 2 * g
        if p == 0:
            return [(d, 0, 0, v, 1) for v in ((0, 1), (2, 3, 4, 5), ())[g] for d in range(2)]
        if p == 1:
            return [(0, 0, 1, u, 2)]
        if p == 2:
            return [(d, 0, 2, u, 2) for d in range(2)]
        return [(1, 0, 3, u, 2)] + ([], [(0, 0, 3, 3, 1)], [(0, 0, 3, 4, 2)])[g]

    def far_of(p, g):
        u = 2 * g
        if p == 0:
            return ([], [(0, 1, 3, 3, 1)], [(0, 1, 3, 4, 2)])[g]
        if p == 1:
            return [(0, 1, 0, v, 1) for v in ((0, 1), (3, 4, 5), ())[g]] + [(1, 1, 2, u, 2)]
        if p == 2:
            return ([(1, 1, 3, 0, 2)], [(1, 1, 3, 2, 1)], [])[g]
        return [(1, 1, 0, 2, 1)] if g == 1 else []

    def into(table, p, g):
        return [t for t in table((p + 3) % 4, g) if t[0] == 0] + [
            t for t in table((p + 1) % 4, g) if t[0] == 1
        ]

    def each_place(f):
        for p in range(4):

            @pl.when(place == p)
            def _():
                f(p)

    def a_ring(d, i, slot):
        half = (d + c + (1 if 3 <= i < 6 else 0)) % 2
        rows = acol.at[slot, pl.ds(pl.multiple_of(half * (NG * H), H) + (i % 3) * H, H)]
        return remote(rows, rows, ns.at[d, i], nr.at[d, i], {"row": fwd if d == 0 else bwd})

    def a_out(i):
        slots = (before, after) if i >= 6 else (place, place)
        return [a_ring(d, i, slots[d]) for d in range(2)]

    def a_in(i):
        slots = (across, across) if i >= 6 else (before, after)
        return [a_ring(d, i, slots[d]) for d in range(2)]

    def both(make, g):
        return [make(d, g) for d in range(2)]

    def start(copies):
        for copy in copies:
            copy.start()

    def arrived(copies):
        for copy in copies:
            copy.wait_recv()

    def mate(g):
        rows = pl.ds(g * G, G)
        return remote(xcol.at[1, rows], xcol.at[1, rows], ms.at[g], mr.at[g], {"col": partner})

    def corner():
        return remote(xcol.at[3, :, pl.ds(0, NG * H)], zx, cs.at[0], cr.at[0], {"col": other_partner})

    def x_near(act, g):
        each_place(lambda p: [act(ring(*t)) for t in near_of(p, g)])

    def x_far(act, g):
        each_place(lambda p: [act(ring(*t)) for t in far_of(p, g)])

    def x_near_in(g):
        def land(p):
            for t in into(near_of, p, g):
                ring(*t).wait_recv()
            if p == 0:
                mate(g).wait_recv()
            if p == 2:
                mate(g).start()

        each_place(land)

    def x_far_in(g):
        def land(p):
            for t in into(far_of, p, g):
                ring(*t).wait_recv()
            if p == 3:
                mate(g).wait_recv()

        each_place(land)

    def mirror():
        for u in range(NU - 1):
            v = slice((u + 1) * H, N)
            xcol[0, u * H : (u + 1) * H, v] = xcol[0, v, u * H : (u + 1) * H].T

    def begin(copy):
        copy.start()

    row_partner = remote(acol.at[place], arow.at[0], ws.at[0], wr.at[0], {"col": partner})

    def a_begin(d, units, where):
        for p in where:

            @pl.when(place == p)
            def _():
                for i in units:
                    a_ring(d, i, p).start()

    def row_other(g):
        rows = pl.ds(g * G, G)
        return remote(acol.at[place, rows], arow.at[1, rows], ws.at[1 + g], wr.at[1 + g], {"col": other})

    def row_forward(g):
        rows = pl.ds(g * G, G)
        return remote(arow.at[1, rows], arow.at[2, rows], ws.at[4 + g], wr.at[4 + g], {"col": partner})

    load_x.wait()
    for g in range(NG):
        x_near(begin, g)

    @pl.when(place == 1)
    def _():
        for g in range(NG):
            mate(g).start()

    load_a.wait()
    for g in range(NG):
        row_other(g).start()
    row_partner.start()

    a_begin(0, (0, 1, 2), (0,))


    def convert(ref, r0, j):
        hi, lo = split(ref[pl.ds(r0, G), :])
        for k in range(NU):
            arh[j, k, pl.ds(r0, G), :] = hi[:, k * H : (k + 1) * H]
            arl[j, k, pl.ds(r0, G), :] = lo[:, k * H : (k + 1) * H]

    @pl.loop(0, NG)
    def _(g):
        convert(acol.at[place], pl.multiple_of(g * G, G), c)

    row_partner.wait_recv()

    @pl.loop(0, NG)
    def _(g):
        convert(arow.at[0], pl.multiple_of(g * G, G), partner)

    def block_of(s):
        return (c + sign * s + 4) % 4

    def pair(ref, j, u):
        return jnp.concatenate([ref[j, u[0]], ref[j, u[1]]], axis=1)

    def split_unit(ref, s, u, at):
        hi, lo = split(ref[s, pl.ds(pl.multiple_of(u * H, H), H), :])
        ch[at * H : (at + 1) * H, :] = hi
        cl[at * H : (at + 1) * H, :] = lo

    def split_units(ref, s, u):
        split_unit(ref, s, u[0], 0)
        split_unit(ref, s, u[1], 1)

    def lanes_of(n):
        return pl.ds(pl.multiple_of(n * G, G), G)

    def add_product(out, j, u, unroll=False):
        @pl.loop(0, NG, unroll=unroll)
        def _(n):
            lanes = lanes_of(n)
            out[:, lanes] += dot3(pair(arh, j, u), pair(arl, j, u), ch[:, lanes], cl[:, lanes], NN)

    def y_step(s, g):
        with jax.named_scope("y"):
            u = (2 * g, 2 * g + 1)
            split_units(xcol, s, u)
            flipped = jnp.logical_and(s == 1, place % 3 == 0)
            j = block_of(s)

            @pl.when(jnp.logical_not(flipped))
            def _():
                add_product(xo, j, u, True)

            @pl.when(flipped)
            def _():
                @pl.loop(0, NG)
                def _(k):
                    v = (2 * k, 2 * k + 1)
                    lanes = lanes_of(k)
                    xo[:, lanes_of(g)] += dot3(pair(arh, j, v), pair(arl, j, v), ch[:, lanes], cl[:, lanes], NT)

    def y_near(g):
        @pl.loop(0, 2)
        def _(n):
            y_step((place + 3 + 2 * n) % 4, g)

    def arrive(i):
        with jax.named_scope("ring"):
            arrived(a_in(i))

    def row_in(g):
        with jax.named_scope("row"):
            row_other(g).wait_recv()
            row_forward(g).start()
            convert(arow.at[1], g * G, other)
            row_forward(g).wait_recv()
            convert(arow.at[2], g * G, other_partner)

    xo[...] = jnp.zeros_like(xo)
    a2[...] = jnp.zeros_like(a2)

    with jax.named_scope("x0"):
        x_near_in(0)
    x_far(begin, 0)
    row_in(0)
    with jax.named_scope("x1"):
        x_near_in(1)
    x_far(begin, 1)
    a_begin(0, (0,), (1, 2))
    a_begin(1, (0,), (2, 3))
    row_in(1)
    with jax.named_scope("x2"):
        x_near_in(2)
    x_far(begin, 2)


    @pl.when(place == 3)
    def _():
        corner().start()

    a_begin(0, (1, 2), (1, 2))
    a_begin(1, (1, 2), (2, 3))
    a_begin(1, (0,), (0,))
    row_in(2)
    a_begin(0, (0, 1, 2), (3,))
    a_begin(1, (1, 2), (0,))
    a_begin(1, (0, 1, 2), (1,))

    @pl.when(place % 2 == 1)
    def _():
        mirror()

    @pl.loop(0, NG)
    def _(g):
        y_step(place, g)

    y_near(2)
    with jax.named_scope("xfar"):
        for g in range(NG):
            x_far_in(g)

        @pl.when(place == 2)
        def _():
            mirror()

    @pl.loop(0, NG)
    def _(g):
        y_step(across, g)

    arrive(0)
    start(a_out(6))
    with jax.named_scope("corner"):

        @pl.when(place == 0)
        def _():
            corner().wait_recv()
            xcol[3, : NG * H, :] = zx[...].T

    @pl.loop(0, 2)
    def _(g):
        y_near(g)

    @pl.loop(0, NG)
    def _(m):
        rows = pl.ds(pl.multiple_of(m * G, G), G)
        hi, lo = split(xo[rows, :])
        yh[rows, :] = hi
        yl[rows, :] = lo

    left, right = (place + 4 - sign) % 4, (place + 4 + sign) % 4

    def to_partner(q, u):
        return remote(part.at[q, u], precv.at[q, u], ps.at[q, u], pr.at[q, u], {"col": partner})

    def to_other(u):
        return remote(part.at[3, u], pzrecv.at[u], zs.at[u], zr.at[u], {"col": other})

    def role(s):
        j = block_of(s)
        q = (j // 2 + c // 2) % 2
        return q, (j + c) % 2 == 0

    def partial(s, u):
        with jax.named_scope("p"):
            for k in range(2):
                split_unit(acol, s[k], u[k], k)
            value = dot3(yh[...], yl[...], ch[...], cl[...], NT)
            for k in range(2):
                q, mine = role(s[k])
                part[q + 2 * mine.astype(jnp.int32), u[k]] = value[:, k * H : (k + 1) * H]

    def hand_over(s, u):
        for k in range(2):
            q, mine = role(s[k])

            @pl.when(jnp.logical_not(mine))
            def _():
                to_partner(q, u[k]).start()

    def collect(s, u):
        for k in range(2):
            q, mine = role(s[k])

            @pl.when(mine)
            def _():
                with jax.named_scope("pwait"):
                    to_partner(q, u[k]).wait_recv()
                part[2 + q, u[k]] += precv[q, u[k]]

                @pl.when(q == 1)
                def _():
                    to_other(u[k]).start()

    odd = (y + c) % 2 == 1
    from_left = role(left)[0] == 1
    last_s = jnp.where(from_left, left, right), jnp.where(from_left, right, left)
    last_u = jnp.where(from_left, 5, 2), jnp.where(from_left, 2, 5)

    def half_to_partner(k, h):
        q, rows = 1 - k, pl.ds(h * (N // 2), N // 2)
        return remote(
            part.at[q, last_u[k], rows],
            precv.at[q, last_u[k], rows],
            hs.at[k, h],
            hr.at[k, h],
            {"col": partner},
        )

    def half_to_other(u, h):
        rows = pl.ds(h * (N // 2), N // 2)
        return remote(part.at[3, u, rows], pzrecv.at[u, rows], hs.at[2, h], hr.at[2, h], {"col": other})

    def last_sums():
        for k in range(2):
            split_unit(acol, last_s[k], last_u[k], k)
        for h in range(2):
            rows = slice(h * (N // 2), (h + 1) * (N // 2))
            value = dot3(yh[rows, :], yl[rows, :], ch[...], cl[...], NT)
            for k in range(2):
                part[1 - k + 2 * odd.astype(jnp.int32), last_u[k], rows] = value[:, k * H : (k + 1) * H]

            @pl.when(jnp.logical_not(odd))
            def _():
                for k in range(2):
                    half_to_partner(k, h).start()

    def last_collect(k):
        @pl.when(odd)
        def _():
            for h in range(2):
                rows = slice(h * (N // 2), (h + 1) * (N // 2))
                with jax.named_scope("pwait"):
                    half_to_partner(k, h).wait_recv()
                part[3 - k, last_u[k], rows] += precv[1 - k, last_u[k], rows]
                if k == 0:
                    half_to_other(last_u[0], h).start()

    def square(s, u):
        with jax.named_scope("a2"):
            split_units(acol, s, u)
            add_product(a2, block_of(s), u)

    def sums(s, u):
        partial(s, u)
        hand_over(s, u)

    def stage(s, u, meanwhile):
        sums(s, u)
        square(*meanwhile)
        collect(s, u)

    own, sides, far_side = (place, place), (left, right), (across, across)
    arrive(1)
    start(a_out(7))
    sums(sides, (0, 3))
    sums(sides, (1, 4))
    collect(sides, (0, 3))
    arrive(2)
    for i in (8, 3, 4, 5):
        start(a_out(i))
    sums(sides, (2, 5))
    collect(sides, (1, 4))
    sums(own, (0, 3))
    collect(sides, (2, 5))
    sums(own, (1, 4))
    collect(own, (0, 3))
    sums(own, (2, 5))
    collect(own, (1, 4))
    arrive(6)
    sums(far_side, (0, 3))
    collect(own, (2, 5))
    square(place, (0, 1))
    collect(far_side, (0, 3))
    square(place, (2, 3))
    arrive(7)
    stage(far_side, (1, 4), (place, (4, 5)))
    square(left, (0, 1))
    arrive(8)
    stage(far_side, (2, 5), (right, (3, 4)))
    square(across, (0, 3))
    arrive(3)
    stage(sides, (3, 0), (across, (1, 4)))
    square(across, (2, 5))
    arrive(4)
    stage(sides, (4, 1), (left, (2, 3)))
    arrive(5)
    with jax.named_scope("p"):
        last_sums()
    last_collect(0)
    square(right, (5, 0))
    last_collect(1)
    square(left, (4, 5))
    square(right, (1, 2))

    for u in (0, 3, 1, 4, 2, 5):
        halves = jnp.logical_and(odd, u == jnp.where((y - c + 4) % 4 == 1, 5, 2))
        with jax.named_scope("z"):

            @pl.when(jnp.logical_not(halves))
            def _():
                to_other(u).wait_recv()

            @pl.when(halves)
            def _():
                for h in range(2):
                    half_to_other(u, h).wait_recv()

        lanes = slice(u * H, (u + 1) * H)
        xo[:, lanes] = xcol[place, :, lanes] + (part[2, u] + pzrecv[u])

    def sent(copy):
        copy.wait_send()

    for g in range(NG):
        x_near(sent, g)
        x_far(sent, g)
        row_other(g).wait_send()
        row_forward(g).wait_send()

    for i in range(9):
        for copy in a_out(i):
            copy.wait_send()

    for u in range(NU):
        for k in range(2):

            @pl.when(jnp.logical_or(odd, u != last_u[k]))
            def _():
                to_partner(1 - k, u).wait_send()

        @pl.when(jnp.logical_or(jnp.logical_not(odd), u != last_u[0]))
        def _():
            to_other(u).wait_send()

    for h in range(2):

        @pl.when(odd)
        def _():
            half_to_other(last_u[0], h).wait_send()

        @pl.when(jnp.logical_not(odd))
        def _():
            for k in range(2):
                half_to_partner(k, h).wait_send()

    @pl.when(jnp.logical_or(place == 1, place == 2))
    def _():
        for g in range(NG):
            mate(g).wait_send()

    @pl.when(place == 3)
    def _():
        corner().wait_send()

    row_partner.wait_send()


def flush(xo, a2, xo_hbm, a2_hbm, sem):
    copies = [
        pltpu.make_async_copy(src, dst, sem.at[i])
        for i, (src, dst) in enumerate(((xo, xo_hbm), (a2, a2_hbm)))
    ]
    for copy in copies:
        copy.start()
    for copy in copies:
        copy.wait()


def solution(mesh):
    def body(a, x):
        block = pltpu.VMEM((N, N), F32)
        dma = pltpu.SemaphoreType.DMA
        xo, a2 = pl.pallas_call(
            kernel,
            out_shape=(block, block),
            in_specs=[pl.BlockSpec(memory_space=pl.ANY)] * 2,
            out_specs=[pl.BlockSpec(memory_space=pltpu.VMEM)] * 2,
            scratch_shapes=[
                pltpu.VMEM((4, N, N), F32),
                pltpu.VMEM((4, N, N), F32),
                pltpu.VMEM((3, N, N), F32),
                pltpu.VMEM((4, NU, N, H), BF),
                pltpu.VMEM((4, NU, N, H), BF),
                pltpu.VMEM((N, N), BF),
                pltpu.VMEM((N, N), BF),
                pltpu.VMEM((G, N), BF),
                pltpu.VMEM((G, N), BF),
                pltpu.VMEM((4, NU, N, H), F32),
                pltpu.VMEM((2, NU, N, H), F32),
                pltpu.VMEM((NU, N, H), F32),
                pltpu.VMEM((N, NG * H), F32),
                dma((2,)),
                dma((2, 2, NU)),
                dma((2, 2, NU)),
                dma((2, 9)),
                dma((2, 9)),
                dma((NG,)),
                dma((NG,)),
                dma((1,)),
                dma((1,)),
                dma((7,)),
                dma((7,)),
                dma((2, NU)),
                dma((2, NU)),
                dma((NU,)),
                dma((NU,)),
                dma((3, 2)),
                dma((3, 2)),
            ],
            compiler_params=pltpu.CompilerParams(
                collective_id=0, has_side_effects=True, vmem_limit_bytes=57 * 2**20
            ),
            cost_estimate=pl.CostEstimate(flops=32614907904, bytes_accessed=9437184, transcendentals=0),
        )(a, x)
        out = jax.ShapeDtypeStruct((N, N), F32)
        return pl.pallas_call(
            flush,
            out_shape=(out, out),
            in_specs=[pl.BlockSpec(memory_space=pltpu.VMEM)] * 2,
            out_specs=[pl.BlockSpec(memory_space=pl.ANY)] * 2,
            scratch_shapes=[dma((2,))],
            compiler_params=pltpu.CompilerParams(vmem_limit_bytes=2**20),
            cost_estimate=pl.CostEstimate(flops=0, bytes_accessed=9437184, transcendentals=0),
        )(xo, a2)

    spec = P(("eq", "row"), "col")
    return jax.shard_map(
        body, mesh=mesh, in_specs=(spec, spec), out_specs=(spec, spec), check_vma=False
    )
```

```python
import jax
import jax.numpy as jnp
from jax import lax
from jax.experimental import pallas as pl
from jax.experimental.pallas import tpu as pltpu
from jax.sharding import PartitionSpec as P

N = 768
G = 256
NG = N // G
H = G // 2
NU = 2 * NG
BF = jnp.bfloat16
F32 = jnp.float32


def split(x):
    hi = x.astype(BF)
    lo = (x - hi.astype(F32)).astype(BF)
    return hi, lo


def dot(a, b, contract):
    return lax.dot_general(a, b, (contract, ((), ())), preferred_element_type=F32)


def dot3(ah, al, bh, bl, contract):
    return dot(ah, bh, contract) + (dot(ah, bl, contract) + dot(al, bh, contract))


NN = ((1,), (0,))
NT = ((1,), (1,))


def kernel(
    a_hbm,
    x_hbm,
    xo,
    a2,
    xcol,
    acol,
    arow,
    arh,
    arl,
    yh,
    yl,
    ch,
    cl,
    part,
    precv,
    pzrecv,
    zx,
    lsem,
    rs,
    rr,
    ns,
    nr,
    ms,
    mr,
    cs,
    cr,
    ws,
    wr,
    ps,
    pr,
    zs,
    zr,
    hs,
    hr,
):
    y = lax.axis_index("row")
    c = lax.axis_index("col")
    partner = c + 1 - 2 * (c % 2)
    other = (c + 2) % 4
    other_partner = (partner + 2) % 4

    sign = 1 - 2 * (c % 2)
    place = ((y - c) * sign + 4) % 4
    load_a = pltpu.make_async_copy(a_hbm, acol.at[place], lsem.at[0])
    load_x = pltpu.make_async_copy(x_hbm, xcol.at[place], lsem.at[1])
    load_x.start()
    load_a.start()

    barrier = pltpu.get_barrier_semaphore()
    for where in ({"row": (y + 1) % 4}, {"row": (y + 3) % 4}, {"col": partner}, {"col": other}, {"col": other_partner}):
        pl.semaphore_signal(barrier, inc=1, device_id=where, device_id_type=pl.DeviceIdType.MESH)
    pl.semaphore_wait(barrier, 5)

    def remote(src, dst, send, recv, where):
        return pltpu.make_async_remote_copy(
            src_ref=src,
            dst_ref=dst,
            send_sem=send,
            recv_sem=recv,
            device_id=where,
            device_id_type=pl.DeviceIdType.MESH,
        )

    fwd, bwd = (y + sign + 4) % 4, (y - sign + 4) % 4
    before, after, across = (place + 3) % 4, (place + 1) % 4, (place + 2) % 4

    def ring(d, kind, slot, u, n=2):
        part = xcol.at[slot, pl.ds(u * H, n * H), pl.ds(0, (u + n) * H if slot == 0 else N)]
        return remote(part, part, rs.at[d, kind, u], rr.at[d, kind, u], {"row": fwd if d == 0 else bwd})

    def near_of(p, g):
        u = 2 * g
        if p == 0:
            return [(d, 0, 0, v, 1) for v in ((0, 1), (2, 3, 4, 5), ())[g] for d in range(2)]
        if p == 1:
            return [(0, 0, 1, u, 2)]
        if p == 2:
            return [(d, 0, 2, u, 2) for d in range(2)]
        return [(1, 0, 3, u, 2)] + ([], [(0, 0, 3, 3, 1)], [(0, 0, 3, 4, 2)])[g]

    def far_of(p, g):
        u = 2 * g
        if p == 0:
            return ([], [(0, 1, 3, 3, 1)], [(0, 1, 3, 4, 2)])[g]
        if p == 1:
            return [(0, 1, 0, v, 1) for v in ((0, 1), (3, 4, 5), ())[g]] + [(1, 1, 2, u, 2)]
        if p == 2:
            return ([(1, 1, 3, 0, 2)], [(1, 1, 3, 2, 1)], [])[g]
        return [(1, 1, 0, 2, 1)] if g == 1 else []

    def into(table, p, g):
        return [t for t in table((p + 3) % 4, g) if t[0] == 0] + [
            t for t in table((p + 1) % 4, g) if t[0] == 1
        ]

    def each_place(f):
        for p in range(4):

            @pl.when(place == p)
            def _():
                f(p)

    def a_ring(d, i, slot):
        half = (d + c + (1 if 3 <= i < 6 else 0)) % 2
        rows = acol.at[slot, pl.ds(pl.multiple_of(half * (NG * H), H) + (i % 3) * H, H)]
        return remote(rows, rows, ns.at[d, i], nr.at[d, i], {"row": fwd if d == 0 else bwd})

    def a_out(i):
        slots = (before, after) if i >= 6 else (place, place)
        return [a_ring(d, i, slots[d]) for d in range(2)]

    def a_in(i):
        slots = (across, across) if i >= 6 else (before, after)
        return [a_ring(d, i, slots[d]) for d in range(2)]

    def both(make, g):
        return [make(d, g) for d in range(2)]

    def start(copies):
        for copy in copies:
            copy.start()

    def arrived(copies):
        for copy in copies:
            copy.wait_recv()

    def mate(g):
        rows = pl.ds(g * G, G)
        return remote(xcol.at[1, rows], xcol.at[1, rows], ms.at[g], mr.at[g], {"col": partner})

    def corner():
        return remote(xcol.at[3, :, pl.ds(0, NG * H)], zx, cs.at[0], cr.at[0], {"col": other_partner})

    def x_near(act, g):
        each_place(lambda p: [act(ring(*t)) for t in near_of(p, g)])

    def x_far(act, g):
        each_place(lambda p: [act(ring(*t)) for t in far_of(p, g)])

    def x_near_in(g):
        def land(p):
            for t in into(near_of, p, g):
                ring(*t).wait_recv()
            if p == 0:
                mate(g).wait_recv()
            if p == 2:
                mate(g).start()

        each_place(land)

    def x_far_in(g):
        def land(p):
            for t in into(far_of, p, g):
                ring(*t).wait_recv()
            if p == 3:
                mate(g).wait_recv()

        each_place(land)

    def mirror():
        for u in range(NU - 1):
            v = slice((u + 1) * H, N)
            xcol[0, u * H : (u + 1) * H, v] = xcol[0, v, u * H : (u + 1) * H].T

    def begin(copy):
        copy.start()

    row_partner = remote(acol.at[place], arow.at[0], ws.at[0], wr.at[0], {"col": partner})

    def a_begin(d, units, where):
        for p in where:

            @pl.when(place == p)
            def _():
                for i in units:
                    a_ring(d, i, p).start()

    def row_other(g):
        rows = pl.ds(g * G, G)
        return remote(acol.at[place, rows], arow.at[1, rows], ws.at[1 + g], wr.at[1 + g], {"col": other})

    def row_forward(g):
        rows = pl.ds(g * G, G)
        return remote(arow.at[1, rows], arow.at[2, rows], ws.at[4 + g], wr.at[4 + g], {"col": partner})

    load_x.wait()
    for g in range(NG):
        x_near(begin, g)

    @pl.when(place == 1)
    def _():
        for g in range(NG):
            mate(g).start()

    load_a.wait()
    for g in range(NG):
        row_other(g).start()
    row_partner.start()

    a_begin(0, (0, 1, 2), (0,))


    def convert(ref, r0, j):
        hi, lo = split(ref[pl.ds(r0, G), :])
        for k in range(NU):
            arh[j, k, pl.ds(r0, G), :] = hi[:, k * H : (k + 1) * H]
            arl[j, k, pl.ds(r0, G), :] = lo[:, k * H : (k + 1) * H]

    @pl.loop(0, NG)
    def _(g):
        convert(acol.at[place], pl.multiple_of(g * G, G), c)

    row_partner.wait_recv()

    @pl.loop(0, NG)
    def _(g):
        convert(arow.at[0], pl.multiple_of(g * G, G), partner)

    def block_of(s):
        return (c + sign * s + 4) % 4

    def pair(ref, j, u):
        return jnp.concatenate([ref[j, u[0]], ref[j, u[1]]], axis=1)

    def split_unit(ref, s, u, at):
        hi, lo = split(ref[s, pl.ds(pl.multiple_of(u * H, H), H), :])
        ch[at * H : (at + 1) * H, :] = hi
        cl[at * H : (at + 1) * H, :] = lo

    def split_units(ref, s, u):
        split_unit(ref, s, u[0], 0)
        split_unit(ref, s, u[1], 1)

    def lanes_of(n):
        return pl.ds(pl.multiple_of(n * G, G), G)

    def add_product(out, j, u, unroll=False):
        @pl.loop(0, NG, unroll=unroll)
        def _(n):
            lanes = lanes_of(n)
            out[:, lanes] += dot3(pair(arh, j, u), pair(arl, j, u), ch[:, lanes], cl[:, lanes], NN)

    def y_step(s, g):
        with jax.named_scope("y"):
            u = (2 * g, 2 * g + 1)
            split_units(xcol, s, u)
            flipped = jnp.logical_and(s == 1, place % 3 == 0)
            j = block_of(s)

            @pl.when(jnp.logical_not(flipped))
            def _():
                add_product(xo, j, u, True)

            @pl.when(flipped)
            def _():
                @pl.loop(0, NG)
                def _(k):
                    v = (2 * k, 2 * k + 1)
                    lanes = lanes_of(k)
                    xo[:, lanes_of(g)] += dot3(pair(arh, j, v), pair(arl, j, v), ch[:, lanes], cl[:, lanes], NT)

    def y_near(g):
        @pl.loop(0, 2)
        def _(n):
            y_step((place + 3 + 2 * n) % 4, g)

    def arrive(i):
        with jax.named_scope("ring"):
            arrived(a_in(i))

    def row_in(g):
        with jax.named_scope("row"):
            row_other(g).wait_recv()
            row_forward(g).start()
            convert(arow.at[1], g * G, other)
            row_forward(g).wait_recv()
            convert(arow.at[2], g * G, other_partner)

    xo[...] = jnp.zeros_like(xo)
    a2[...] = jnp.zeros_like(a2)

    with jax.named_scope("x0"):
        x_near_in(0)
    x_far(begin, 0)
    row_in(0)
    with jax.named_scope("x1"):
        x_near_in(1)
    x_far(begin, 1)
    a_begin(0, (0,), (1, 2))
    a_begin(1, (0,), (2, 3))
    row_in(1)
    with jax.named_scope("x2"):
        x_near_in(2)
    x_far(begin, 2)


    @pl.when(place == 3)
    def _():
        corner().start()

    a_begin(0, (1, 2), (1, 2))
    a_begin(1, (1, 2), (2, 3))
    a_begin(1, (0,), (0,))
    row_in(2)
    a_begin(0, (0, 1, 2), (3,))
    a_begin(1, (1, 2), (0,))
    a_begin(1, (0, 1, 2), (1,))

    @pl.when(place % 2 == 1)
    def _():
        mirror()

    @pl.loop(0, NG)
    def _(g):
        y_step(place, g)

    y_near(2)
    with jax.named_scope("xfar"):
        for g in range(NG):
            x_far_in(g)

        @pl.when(place == 2)
        def _():
            mirror()

    @pl.loop(0, NG)
    def _(g):
        y_step(across, g)

    arrive(0)
    start(a_out(6))
    with jax.named_scope("corner"):

        @pl.when(place == 0)
        def _():
            corner().wait_recv()
            xcol[3, : NG * H, :] = zx[...].T

    @pl.loop(0, 2)
    def _(g):
        y_near(g)

    @pl.loop(0, NG)
    def _(m):
        rows = pl.ds(pl.multiple_of(m * G, G), G)
        hi, lo = split(xo[rows, :])
        yh[rows, :] = hi
        yl[rows, :] = lo

    left, right = (place + 4 - sign) % 4, (place + 4 + sign) % 4

    def to_partner(q, u):
        return remote(part.at[q, u], precv.at[q, u], ps.at[q, u], pr.at[q, u], {"col": partner})

    def to_other(u):
        return remote(part.at[3, u], pzrecv.at[u], zs.at[u], zr.at[u], {"col": other})

    def role(s):
        j = block_of(s)
        q = (j // 2 + c // 2) % 2
        return q, (j + c) % 2 == 0

    def partial(s, u):
        with jax.named_scope("p"):
            for k in range(2):
                split_unit(acol, s[k], u[k], k)
            value = dot3(yh[...], yl[...], ch[...], cl[...], NT)
            for k in range(2):
                q, mine = role(s[k])
                part[q + 2 * mine.astype(jnp.int32), u[k]] = value[:, k * H : (k + 1) * H]

    def hand_over(s, u):
        for k in range(2):
            q, mine = role(s[k])

            @pl.when(jnp.logical_not(mine))
            def _():
                to_partner(q, u[k]).start()

    def collect(s, u):
        for k in range(2):
            q, mine = role(s[k])

            @pl.when(mine)
            def _():
                with jax.named_scope("pwait"):
                    to_partner(q, u[k]).wait_recv()
                part[2 + q, u[k]] += precv[q, u[k]]

                @pl.when(q == 1)
                def _():
                    to_other(u[k]).start()

    odd = (y + c) % 2 == 1
    from_left = role(left)[0] == 1
    last_s = jnp.where(from_left, left, right), jnp.where(from_left, right, left)
    last_u = jnp.where(from_left, 5, 2), jnp.where(from_left, 2, 5)

    def crossing(u, v):
        return jnp.where(from_left, u, v), jnp.where(from_left, v, u)

    def half_to_partner(k, h):
        q, rows = 1 - k, pl.ds(h * (N // 2), N // 2)
        return remote(
            part.at[q, last_u[k], rows],
            precv.at[q, last_u[k], rows],
            hs.at[k, h],
            hr.at[k, h],
            {"col": partner},
        )

    def half_to_other(u, h):
        rows = pl.ds(h * (N // 2), N // 2)
        return remote(part.at[3, u, rows], pzrecv.at[u, rows], hs.at[2, h], hr.at[2, h], {"col": other})

    def last_sums():
        for k in range(2):
            split_unit(acol, last_s[k], last_u[k], k)
        value = dot3(yh[...], yl[...], ch[...], cl[...], NT)
        for k in range(2):
            part[1 - k + 2 * odd.astype(jnp.int32), last_u[k]] = value[:, k * H : (k + 1) * H]

        @pl.when(jnp.logical_not(odd))
        def _():
            for k in range(2):
                for h in range(2):
                    half_to_partner(k, h).start()

    def last_collect(k):
        @pl.when(odd)
        def _():
            for h in range(2):
                rows = slice(h * (N // 2), (h + 1) * (N // 2))
                with jax.named_scope("pwait"):
                    half_to_partner(k, h).wait_recv()
                part[3 - k, last_u[k], rows] += precv[1 - k, last_u[k], rows]
                if k == 0:
                    half_to_other(last_u[0], h).start()

    def square(s, u):
        with jax.named_scope("a2"):
            split_units(acol, s, u)
            add_product(a2, block_of(s), u)

    def sums(s, u):
        partial(s, u)
        hand_over(s, u)

    def stage(s, u, meanwhile):
        sums(s, u)
        square(*meanwhile)
        collect(s, u)

    own, far_side = (place, place), (across, across)
    arrive(1)
    start(a_out(7))
    sums(last_s, crossing(0, 3))
    sums(last_s, crossing(1, 4))
    collect(last_s, crossing(0, 3))
    arrive(2)
    for i in (8, 3, 4, 5):
        start(a_out(i))
    sums(last_s, crossing(2, 5))
    collect(last_s, crossing(1, 4))
    sums(own, (0, 3))
    collect(last_s, crossing(2, 5))
    sums(own, (1, 4))
    collect(own, (0, 3))
    sums(own, (2, 5))
    collect(own, (1, 4))
    arrive(6)
    sums(far_side, (0, 3))
    collect(own, (2, 5))
    square(place, (0, 1))
    collect(far_side, (0, 3))
    square(place, (2, 3))
    arrive(7)
    stage(far_side, (1, 4), (place, (4, 5)))
    square(left, (0, 1))
    arrive(8)
    stage(far_side, (2, 5), (right, (3, 4)))
    square(across, (0, 3))
    arrive(3)
    stage(last_s, crossing(3, 0), (across, (1, 4)))
    square(across, (2, 5))
    arrive(4)
    stage(last_s, crossing(4, 1), (left, (2, 3)))
    arrive(5)
    with jax.named_scope("p"):
        last_sums()
    last_collect(0)
    square(right, (5, 0))
    last_collect(1)
    square(left, (4, 5))
    square(right, (1, 2))

    for u in (0, 3, 1, 4, 2, 5):
        halves = jnp.logical_and(odd, u == jnp.where((y - c + 4) % 4 == 1, 5, 2))
        with jax.named_scope("z"):

            @pl.when(jnp.logical_not(halves))
            def _():
                to_other(u).wait_recv()

            @pl.when(halves)
            def _():
                for h in range(2):
                    half_to_other(u, h).wait_recv()

        lanes = slice(u * H, (u + 1) * H)
        xo[:, lanes] = xcol[place, :, lanes] + (part[2, u] + pzrecv[u])

    def sent(copy):
        copy.wait_send()

    for g in range(NG):
        x_near(sent, g)
        x_far(sent, g)
        row_other(g).wait_send()
        row_forward(g).wait_send()

    for i in range(9):
        for copy in a_out(i):
            copy.wait_send()

    for u in range(NU):
        for k in range(2):

            @pl.when(jnp.logical_or(odd, u != last_u[k]))
            def _():
                to_partner(1 - k, u).wait_send()

        @pl.when(jnp.logical_or(jnp.logical_not(odd), u != last_u[0]))
        def _():
            to_other(u).wait_send()

    for h in range(2):

        @pl.when(odd)
        def _():
            half_to_other(last_u[0], h).wait_send()

        @pl.when(jnp.logical_not(odd))
        def _():
            for k in range(2):
                half_to_partner(k, h).wait_send()

    @pl.when(jnp.logical_or(place == 1, place == 2))
    def _():
        for g in range(NG):
            mate(g).wait_send()

    @pl.when(place == 3)
    def _():
        corner().wait_send()

    row_partner.wait_send()


def flush(xo, a2, xo_hbm, a2_hbm, sem):
    copies = [
        pltpu.make_async_copy(src, dst, sem.at[i])
        for i, (src, dst) in enumerate(((xo, xo_hbm), (a2, a2_hbm)))
    ]
    for copy in copies:
        copy.start()
    for copy in copies:
        copy.wait()


def solution(mesh):
    def body(a, x):
        block = pltpu.VMEM((N, N), F32)
        dma = pltpu.SemaphoreType.DMA
        xo, a2 = pl.pallas_call(
            kernel,
            out_shape=(block, block),
            in_specs=[pl.BlockSpec(memory_space=pl.ANY)] * 2,
            out_specs=[pl.BlockSpec(memory_space=pltpu.VMEM)] * 2,
            scratch_shapes=[
                pltpu.VMEM((4, N, N), F32),
                pltpu.VMEM((4, N, N), F32),
                pltpu.VMEM((3, N, N), F32),
                pltpu.VMEM((4, NU, N, H), BF),
                pltpu.VMEM((4, NU, N, H), BF),
                pltpu.VMEM((N, N), BF),
                pltpu.VMEM((N, N), BF),
                pltpu.VMEM((G, N), BF),
                pltpu.VMEM((G, N), BF),
                pltpu.VMEM((4, NU, N, H), F32),
                pltpu.VMEM((2, NU, N, H), F32),
                pltpu.VMEM((NU, N, H), F32),
                pltpu.VMEM((N, NG * H), F32),
                dma((2,)),
                dma((2, 2, NU)),
                dma((2, 2, NU)),
                dma((2, 9)),
                dma((2, 9)),
                dma((NG,)),
                dma((NG,)),
                dma((1,)),
                dma((1,)),
                dma((7,)),
                dma((7,)),
                dma((2, NU)),
                dma((2, NU)),
                dma((NU,)),
                dma((NU,)),
                dma((3, 2)),
                dma((3, 2)),
            ],
            compiler_params=pltpu.CompilerParams(
                collective_id=0, has_side_effects=True, vmem_limit_bytes=57 * 2**20
            ),
            cost_estimate=pl.CostEstimate(flops=32614907904, bytes_accessed=9437184, transcendentals=0),
        )(a, x)
        out = jax.ShapeDtypeStruct((N, N), F32)
        return pl.pallas_call(
            flush,
            out_shape=(out, out),
            in_specs=[pl.BlockSpec(memory_space=pltpu.VMEM)] * 2,
            out_specs=[pl.BlockSpec(memory_space=pl.ANY)] * 2,
            scratch_shapes=[dma((2,))],
            compiler_params=pltpu.CompilerParams(vmem_limit_bytes=2**20),
            cost_estimate=pl.CostEstimate(flops=0, bytes_accessed=9437184, transcendentals=0),
        )(xo, a2)

    spec = P(("eq", "row"), "col")
    return jax.shard_map(
        body, mesh=mesh, in_specs=(spec, spec), out_specs=(spec, spec), check_vma=False
    )
```

```python
import jax
import jax.numpy as jnp
from jax import lax
from jax.experimental import pallas as pl
from jax.experimental.pallas import tpu as pltpu
from jax.sharding import PartitionSpec as P

N = 768
G = 256
NG = N // G
H = G // 2
NU = 2 * NG
BF = jnp.bfloat16
F32 = jnp.float32


def split(x):
    hi = x.astype(BF)
    lo = (x - hi.astype(F32)).astype(BF)
    return hi, lo


def dot(a, b, contract):
    return lax.dot_general(a, b, (contract, ((), ())), preferred_element_type=F32)


def dot3(ah, al, bh, bl, contract):
    return dot(ah, bh, contract) + (dot(ah, bl, contract) + dot(al, bh, contract))


NN = ((1,), (0,))
NT = ((1,), (1,))


def kernel(
    a_hbm,
    x_hbm,
    xo,
    a2,
    xcol,
    acol,
    arow,
    arh,
    arl,
    yh,
    yl,
    ch,
    cl,
    part,
    precv,
    pzrecv,
    zx,
    lsem,
    rs,
    rr,
    ns,
    nr,
    ms,
    mr,
    cs,
    cr,
    ws,
    wr,
    ps,
    pr,
    zs,
    zr,
    hs,
    hr,
):
    y = lax.axis_index("row")
    c = lax.axis_index("col")
    partner = c + 1 - 2 * (c % 2)
    other = (c + 2) % 4
    other_partner = (partner + 2) % 4

    sign = 1 - 2 * (c % 2)
    place = ((y - c) * sign + 4) % 4
    load_a = pltpu.make_async_copy(a_hbm, acol.at[place], lsem.at[0])
    load_x = pltpu.make_async_copy(x_hbm, xcol.at[place], lsem.at[1])
    load_x.start()
    load_a.start()

    barrier = pltpu.get_barrier_semaphore()
    for where in ({"row": (y + 1) % 4}, {"row": (y + 3) % 4}, {"col": partner}, {"col": other}, {"col": other_partner}):
        pl.semaphore_signal(barrier, inc=1, device_id=where, device_id_type=pl.DeviceIdType.MESH)
    pl.semaphore_wait(barrier, 5)

    def remote(src, dst, send, recv, where):
        return pltpu.make_async_remote_copy(
            src_ref=src,
            dst_ref=dst,
            send_sem=send,
            recv_sem=recv,
            device_id=where,
            device_id_type=pl.DeviceIdType.MESH,
        )

    fwd, bwd = (y + sign + 4) % 4, (y - sign + 4) % 4
    before, after, across = (place + 3) % 4, (place + 1) % 4, (place + 2) % 4

    def ring(d, kind, slot, u, n=2):
        part = xcol.at[slot, pl.ds(u * H, n * H), pl.ds(0, (u + n) * H if slot == 0 else N)]
        return remote(part, part, rs.at[d, kind, u], rr.at[d, kind, u], {"row": fwd if d == 0 else bwd})

    def near_of(p, g):
        u = 2 * g
        if p == 0:
            return [(d, 0, 0, v, 1) for v in ((0, 1), (2, 3, 4, 5), ())[g] for d in range(2)]
        if p == 1:
            return [(0, 0, 1, u, 2)]
        if p == 2:
            return [(d, 0, 2, u, 2) for d in range(2)]
        return [(1, 0, 3, u, 2)] + ([], [(0, 0, 3, 3, 1)], [(0, 0, 3, 4, 2)])[g]

    def far_of(p, g):
        u = 2 * g
        if p == 0:
            return ([], [(0, 1, 3, 3, 1)], [(0, 1, 3, 4, 2)])[g]
        if p == 1:
            return [(0, 1, 0, v, 1) for v in ((0, 1), (3, 4, 5), ())[g]] + [(1, 1, 2, u, 2)]
        if p == 2:
            return ([(1, 1, 3, 0, 2)], [(1, 1, 3, 2, 1)], [])[g]
        return [(1, 1, 0, 2, 1)] if g == 1 else []

    def into(table, p, g):
        return [t for t in table((p + 3) % 4, g) if t[0] == 0] + [
            t for t in table((p + 1) % 4, g) if t[0] == 1
        ]

    def each_place(f):
        for p in range(4):

            @pl.when(place == p)
            def _():
                f(p)

    def a_ring(d, i, slot):
        half = (d + c + (1 if 3 <= i < 6 else 0)) % 2
        rows = acol.at[slot, pl.ds(pl.multiple_of(half * (NG * H), H) + (i % 3) * H, H)]
        return remote(rows, rows, ns.at[d, i], nr.at[d, i], {"row": fwd if d == 0 else bwd})

    def a_out(i):
        slots = (before, after) if i >= 6 else (place, place)
        return [a_ring(d, i, slots[d]) for d in range(2)]

    def a_in(i):
        slots = (across, across) if i >= 6 else (before, after)
        return [a_ring(d, i, slots[d]) for d in range(2)]

    def both(make, g):
        return [make(d, g) for d in range(2)]

    def start(copies):
        for copy in copies:
            copy.start()

    def arrived(copies):
        for copy in copies:
            copy.wait_recv()

    def mate(g):
        rows = pl.ds(g * G, G)
        return remote(xcol.at[1, rows], xcol.at[1, rows], ms.at[g], mr.at[g], {"col": partner})

    def corner():
        return remote(xcol.at[3, :, pl.ds(0, NG * H)], zx, cs.at[0], cr.at[0], {"col": other_partner})

    def x_near(act, g):
        each_place(lambda p: [act(ring(*t)) for t in near_of(p, g)])

    def x_far(act, g):
        each_place(lambda p: [act(ring(*t)) for t in far_of(p, g)])

    def x_near_in(g):
        def land(p):
            for t in into(near_of, p, g):
                ring(*t).wait_recv()
            if p == 0:
                mate(g).wait_recv()
            if p == 2:
                mate(g).start()

        each_place(land)

    def x_far_in(g):
        def land(p):
            for t in into(far_of, p, g):
                ring(*t).wait_recv()
            if p == 3:
                mate(g).wait_recv()

        each_place(land)

    def mirror():
        for u in range(NU - 1):
            v = slice((u + 1) * H, N)
            xcol[0, u * H : (u + 1) * H, v] = xcol[0, v, u * H : (u + 1) * H].T

    def begin(copy):
        copy.start()

    row_partner = remote(acol.at[place], arow.at[0], ws.at[0], wr.at[0], {"col": partner})

    def a_begin(d, units, where):
        for p in where:

            @pl.when(place == p)
            def _():
                for i in units:
                    a_ring(d, i, p).start()

    def row_other(g):
        rows = pl.ds(g * G, G)
        return remote(acol.at[place, rows], arow.at[1, rows], ws.at[1 + g], wr.at[1 + g], {"col": other})

    def row_forward(g):
        rows = pl.ds(g * G, G)
        return remote(arow.at[1, rows], arow.at[2, rows], ws.at[4 + g], wr.at[4 + g], {"col": partner})

    load_x.wait()
    for g in range(NG):
        x_near(begin, g)

    @pl.when(place == 1)
    def _():
        for g in range(NG):
            mate(g).start()

    load_a.wait()
    for g in range(NG):
        row_other(g).start()
    row_partner.start()

    a_begin(0, (0, 1, 2), (0,))


    def convert(ref, r0, j):
        hi, lo = split(ref[pl.ds(r0, G), :])
        for k in range(NU):
            arh[j, k, pl.ds(r0, G), :] = hi[:, k * H : (k + 1) * H]
            arl[j, k, pl.ds(r0, G), :] = lo[:, k * H : (k + 1) * H]

    @pl.loop(0, NG)
    def _(g):
        convert(acol.at[place], pl.multiple_of(g * G, G), c)

    row_partner.wait_recv()

    @pl.loop(0, NG)
    def _(g):
        convert(arow.at[0], pl.multiple_of(g * G, G), partner)

    def block_of(s):
        return (c + sign * s + 4) % 4

    def pair(ref, j, u):
        return jnp.concatenate([ref[j, u[0]], ref[j, u[1]]], axis=1)

    def split_unit(ref, s, u, at):
        hi, lo = split(ref[s, pl.ds(pl.multiple_of(u * H, H), H), :])
        ch[at * H : (at + 1) * H, :] = hi
        cl[at * H : (at + 1) * H, :] = lo

    def split_units(ref, s, u):
        split_unit(ref, s, u[0], 0)
        split_unit(ref, s, u[1], 1)

    def lanes_of(n):
        return pl.ds(pl.multiple_of(n * G, G), G)

    def add_product(out, j, u, unroll=False):
        @pl.loop(0, NG, unroll=unroll)
        def _(n):
            lanes = lanes_of(n)
            out[:, lanes] += dot3(pair(arh, j, u), pair(arl, j, u), ch[:, lanes], cl[:, lanes], NN)

    def y_step(s, g):
        with jax.named_scope("y"):
            u = (2 * g, 2 * g + 1)
            split_units(xcol, s, u)
            flipped = jnp.logical_and(s == 1, place % 3 == 0)
            j = block_of(s)

            @pl.when(jnp.logical_not(flipped))
            def _():
                add_product(xo, j, u, True)

            @pl.when(flipped)
            def _():
                @pl.loop(0, NG, unroll=True)
                def _(k):
                    v = (2 * k, 2 * k + 1)
                    lanes = lanes_of(k)
                    xo[:, lanes_of(g)] += dot3(pair(arh, j, v), pair(arl, j, v), ch[:, lanes], cl[:, lanes], NT)

    def y_near(g):
        @pl.loop(0, 2)
        def _(n):
            y_step((place + 3 + 2 * n) % 4, g)

    def arrive(i):
        with jax.named_scope("ring"):
            arrived(a_in(i))

    def row_in(g):
        with jax.named_scope("row"):
            row_other(g).wait_recv()
            row_forward(g).start()
            convert(arow.at[1], g * G, other)
            row_forward(g).wait_recv()
            convert(arow.at[2], g * G, other_partner)

    xo[...] = jnp.zeros_like(xo)
    a2[...] = jnp.zeros_like(a2)

    with jax.named_scope("x0"):
        x_near_in(0)
    x_far(begin, 0)
    row_in(0)
    with jax.named_scope("x1"):
        x_near_in(1)
    x_far(begin, 1)
    a_begin(0, (0,), (1, 2))
    a_begin(1, (0,), (2, 3))
    row_in(1)
    with jax.named_scope("x2"):
        x_near_in(2)
    x_far(begin, 2)


    @pl.when(place == 3)
    def _():
        corner().start()

    a_begin(0, (1, 2), (1, 2))
    a_begin(1, (1, 2), (2, 3))
    a_begin(1, (0,), (0,))
    row_in(2)
    a_begin(0, (0, 1, 2), (3,))
    a_begin(1, (1, 2), (0,))
    a_begin(1, (0, 1, 2), (1,))

    @pl.when(place % 2 == 1)
    def _():
        mirror()

    @pl.loop(0, NG)
    def _(g):
        y_step(place, g)

    y_near(2)
    with jax.named_scope("xfar"):
        for g in range(NG):
            x_far_in(g)

        @pl.when(place == 2)
        def _():
            mirror()

    @pl.loop(0, NG)
    def _(g):
        y_step(across, g)

    arrive(0)
    start(a_out(6))
    with jax.named_scope("corner"):

        @pl.when(place == 0)
        def _():
            corner().wait_recv()
            xcol[3, : NG * H, :] = zx[...].T

    @pl.loop(0, 2)
    def _(g):
        y_near(g)

    @pl.loop(0, NG)
    def _(m):
        rows = pl.ds(pl.multiple_of(m * G, G), G)
        hi, lo = split(xo[rows, :])
        yh[rows, :] = hi
        yl[rows, :] = lo

    left, right = (place + 4 - sign) % 4, (place + 4 + sign) % 4

    def to_partner(q, u):
        return remote(part.at[q, u], precv.at[q, u], ps.at[q, u], pr.at[q, u], {"col": partner})

    def to_other(u):
        return remote(part.at[3, u], pzrecv.at[u], zs.at[u], zr.at[u], {"col": other})

    def role(s):
        j = block_of(s)
        q = (j // 2 + c // 2) % 2
        return q, (j + c) % 2 == 0

    def partial(s, u):
        with jax.named_scope("p"):
            for k in range(2):
                split_unit(acol, s[k], u[k], k)
            value = dot3(yh[...], yl[...], ch[...], cl[...], NT)
            for k in range(2):
                q, mine = role(s[k])
                part[q + 2 * mine.astype(jnp.int32), u[k]] = value[:, k * H : (k + 1) * H]

    def hand_over(s, u):
        for k in range(2):
            q, mine = role(s[k])

            @pl.when(jnp.logical_not(mine))
            def _():
                to_partner(q, u[k]).start()

    def collect(s, u):
        for k in range(2):
            q, mine = role(s[k])

            @pl.when(mine)
            def _():
                with jax.named_scope("pwait"):
                    to_partner(q, u[k]).wait_recv()
                part[2 + q, u[k]] += precv[q, u[k]]

                @pl.when(q == 1)
                def _():
                    to_other(u[k]).start()

    odd = (y + c) % 2 == 1
    from_left = role(left)[0] == 1
    last_s = jnp.where(from_left, left, right), jnp.where(from_left, right, left)
    last_u = jnp.where(from_left, 5, 2), jnp.where(from_left, 2, 5)

    def crossing(u, v):
        return jnp.where(from_left, u, v), jnp.where(from_left, v, u)

    def half_to_partner(k, h):
        q, rows = 1 - k, pl.ds(h * (N // 2), N // 2)
        return remote(
            part.at[q, last_u[k], rows],
            precv.at[q, last_u[k], rows],
            hs.at[k, h],
            hr.at[k, h],
            {"col": partner},
        )

    def half_to_other(u, h):
        rows = pl.ds(h * (N // 2), N // 2)
        return remote(part.at[3, u, rows], pzrecv.at[u, rows], hs.at[2, h], hr.at[2, h], {"col": other})

    def last_sums():
        for k in range(2):
            split_unit(acol, last_s[k], last_u[k], k)
        value = dot3(yh[...], yl[...], ch[...], cl[...], NT)
        for k in range(2):
            part[1 - k + 2 * odd.astype(jnp.int32), last_u[k]] = value[:, k * H : (k + 1) * H]

        @pl.when(jnp.logical_not(odd))
        def _():
            for k in range(2):
                for h in range(2):
                    half_to_partner(k, h).start()

    def last_collect(k):
        @pl.when(odd)
        def _():
            for h in range(2):
                rows = slice(h * (N // 2), (h + 1) * (N // 2))
                with jax.named_scope("pwait"):
                    half_to_partner(k, h).wait_recv()
                part[3 - k, last_u[k], rows] += precv[1 - k, last_u[k], rows]
                if k == 0:
                    half_to_other(last_u[0], h).start()

    def square(s, u):
        with jax.named_scope("a2"):
            split_units(acol, s, u)
            add_product(a2, block_of(s), u)

    def sums(s, u):
        partial(s, u)
        hand_over(s, u)

    def stage(s, u, meanwhile):
        sums(s, u)
        square(*meanwhile)
        collect(s, u)

    own, far_side = (place, place), (across, across)
    arrive(1)
    start(a_out(7))
    sums(last_s, crossing(0, 3))
    sums(last_s, crossing(1, 4))
    collect(last_s, crossing(0, 3))
    arrive(2)
    for i in (8, 3, 4, 5):
        start(a_out(i))
    sums(last_s, crossing(2, 5))
    collect(last_s, crossing(1, 4))
    sums(own, (0, 3))
    collect(last_s, crossing(2, 5))
    sums(own, (1, 4))
    collect(own, (0, 3))
    sums(own, (2, 5))
    collect(own, (1, 4))
    arrive(6)
    sums(far_side, (0, 3))
    collect(own, (2, 5))
    square(place, (0, 1))
    collect(far_side, (0, 3))
    square(place, (2, 3))
    arrive(7)
    stage(far_side, (1, 4), (place, (4, 5)))
    square(left, (0, 1))
    arrive(8)
    stage(far_side, (2, 5), (right, (3, 4)))
    square(across, (0, 3))
    arrive(3)
    stage(last_s, crossing(3, 0), (across, (1, 4)))
    square(across, (2, 5))
    arrive(4)
    stage(last_s, crossing(4, 1), (left, (2, 3)))
    arrive(5)
    with jax.named_scope("p"):
        last_sums()
    last_collect(0)
    square(right, (5, 0))
    last_collect(1)
    square(left, (4, 5))
    square(right, (1, 2))

    for u in (0, 3, 1, 4, 2, 5):
        halves = jnp.logical_and(odd, u == jnp.where((y - c + 4) % 4 == 1, 5, 2))
        with jax.named_scope("z"):

            @pl.when(jnp.logical_not(halves))
            def _():
                to_other(u).wait_recv()

            @pl.when(halves)
            def _():
                for h in range(2):
                    half_to_other(u, h).wait_recv()

        lanes = slice(u * H, (u + 1) * H)
        xo[:, lanes] = xcol[place, :, lanes] + (part[2, u] + pzrecv[u])

    def sent(copy):
        copy.wait_send()

    for g in range(NG):
        x_near(sent, g)
        x_far(sent, g)
        row_other(g).wait_send()
        row_forward(g).wait_send()

    for i in range(9):
        for copy in a_out(i):
            copy.wait_send()

    for u in range(NU):
        for k in range(2):

            @pl.when(jnp.logical_or(odd, u != last_u[k]))
            def _():
                to_partner(1 - k, u).wait_send()

        @pl.when(jnp.logical_or(jnp.logical_not(odd), u != last_u[0]))
        def _():
            to_other(u).wait_send()

    for h in range(2):

        @pl.when(odd)
        def _():
            half_to_other(last_u[0], h).wait_send()

        @pl.when(jnp.logical_not(odd))
        def _():
            for k in range(2):
                half_to_partner(k, h).wait_send()

    @pl.when(jnp.logical_or(place == 1, place == 2))
    def _():
        for g in range(NG):
            mate(g).wait_send()

    @pl.when(place == 3)
    def _():
        corner().wait_send()

    row_partner.wait_send()


def flush(xo, a2, xo_hbm, a2_hbm, sem):
    copies = [
        pltpu.make_async_copy(src, dst, sem.at[i])
        for i, (src, dst) in enumerate(((xo, xo_hbm), (a2, a2_hbm)))
    ]
    for copy in copies:
        copy.start()
    for copy in copies:
        copy.wait()


def solution(mesh):
    def body(a, x):
        block = pltpu.VMEM((N, N), F32)
        dma = pltpu.SemaphoreType.DMA
        xo, a2 = pl.pallas_call(
            kernel,
            out_shape=(block, block),
            in_specs=[pl.BlockSpec(memory_space=pl.ANY)] * 2,
            out_specs=[pl.BlockSpec(memory_space=pltpu.VMEM)] * 2,
            scratch_shapes=[
                pltpu.VMEM((4, N, N), F32),
                pltpu.VMEM((4, N, N), F32),
                pltpu.VMEM((3, N, N), F32),
                pltpu.VMEM((4, NU, N, H), BF),
                pltpu.VMEM((4, NU, N, H), BF),
                pltpu.VMEM((N, N), BF),
                pltpu.VMEM((N, N), BF),
                pltpu.VMEM((G, N), BF),
                pltpu.VMEM((G, N), BF),
                pltpu.VMEM((4, NU, N, H), F32),
                pltpu.VMEM((2, NU, N, H), F32),
                pltpu.VMEM((NU, N, H), F32),
                pltpu.VMEM((N, NG * H), F32),
                dma((2,)),
                dma((2, 2, NU)),
                dma((2, 2, NU)),
                dma((2, 9)),
                dma((2, 9)),
                dma((NG,)),
                dma((NG,)),
                dma((1,)),
                dma((1,)),
                dma((7,)),
                dma((7,)),
                dma((2, NU)),
                dma((2, NU)),
                dma((NU,)),
                dma((NU,)),
                dma((3, 2)),
                dma((3, 2)),
            ],
            compiler_params=pltpu.CompilerParams(
                collective_id=0, has_side_effects=True, vmem_limit_bytes=57 * 2**20
            ),
            cost_estimate=pl.CostEstimate(flops=32614907904, bytes_accessed=9437184, transcendentals=0),
        )(a, x)
        out = jax.ShapeDtypeStruct((N, N), F32)
        return pl.pallas_call(
            flush,
            out_shape=(out, out),
            in_specs=[pl.BlockSpec(memory_space=pltpu.VMEM)] * 2,
            out_specs=[pl.BlockSpec(memory_space=pl.ANY)] * 2,
            scratch_shapes=[dma((2,))],
            compiler_params=pltpu.CompilerParams(vmem_limit_bytes=2**20),
            cost_estimate=pl.CostEstimate(flops=0, bytes_accessed=9437184, transcendentals=0),
        )(xo, a2)

    spec = P(("eq", "row"), "col")
    return jax.shard_map(
        body, mesh=mesh, in_specs=(spec, spec), out_specs=(spec, spec), check_vma=False
    )
```
